8 devices in a mesh: dp: 1 (over z), col: 2 (over y), row: 4 (over x, core).
Axes of the slice: x: 2, y: 2, z: 1, core: 2. Of those that a mesh axis runs over, the one named last changes fastest.
Arguments:
- x_in: bfloat16 [2, 4096, 5120], P(None, ('dp', 'row'), 'col')
- ln_gamma: float32 [5120], P('col')
- w_in: bfloat16 [5120, 20480], P('row', 'col')
- w_out: bfloat16 [20480, 5120], P('row', 'col')
Outputs:
- output: bfloat16 [2, 4096, 5120], P(None, ('dp', 'row'), 'col')
All inputs are finite; a program needn't handle non-finite values.
Results may differ from the reference program's by a relative error of at most 0.00106.
Values are sent between devices in bfloat16 or wider.
A program may use at most 1 GiB of HBM per device.

```python
import jax
import jax.numpy as jnp
from jax import lax

D_MODEL = 5120
D_FF = 20480
MB_TOKENS = 4096
ROW_BLOCK = 1024
LN_EPS = 1e-5
N_BLOCKS = 2 * MB_TOKENS // ROW_BLOCK


def setup_inputs(seed: int = 0, part: int = 0) -> dict:
    base_key = jax.random.key(seed)
    part_key = jax.random.fold_in(base_key, part)
    key_noise, key_off, key_tilt, key_col = jax.random.split(part_key, 4)
    shared_key = jax.random.key(seed + 1)
    key_gamma, key_win, key_wout = jax.random.split(shared_key, 3)
    ramp = jnp.arange(D_MODEL, dtype=jnp.float32) / D_MODEL
    col_scale = (0.4 + 1.2 * ramp) * jax.random.uniform(key_col, (D_MODEL,), jnp.float32, 0.8, 1.2)
    noise = jax.random.normal(key_noise, (2, MB_TOKENS, D_MODEL), jnp.float32)
    row_off = 0.5 * jax.random.normal(key_off, (2, MB_TOKENS, 1), jnp.float32)
    row_tilt = jax.random.normal(key_tilt, (2, MB_TOKENS, 1), jnp.float32)
    x_val = row_off + row_tilt * (ramp - 0.5) + col_scale * noise
    ln_gamma = jax.random.uniform(key_gamma, (D_MODEL,), jnp.float32, 0.5, 1.5)
    w_in = jax.random.normal(key_win, (D_MODEL, D_FF), jnp.float32) * D_MODEL ** -0.5
    w_out = jax.random.normal(key_wout, (D_FF, D_MODEL), jnp.float32) * (1.5 * D_FF ** -0.5)
    return {"x_in": x_val.astype(jnp.bfloat16), "ln_gamma": ln_gamma, "w_in": w_in.astype(jnp.bfloat16), "w_out": w_out.astype(jnp.bfloat16)}


def reference(x_in, ln_gamma, w_in, w_out):
    row_blocks = x_in.reshape(N_BLOCKS, ROW_BLOCK, D_MODEL)

    def one_block(x_blk):
        x_f32 = x_blk.astype(jnp.float32)
        row_mean = jnp.sum(x_f32, axis=-1, keepdims=True) / D_MODEL
        row_var = jnp.sum(x_f32 * x_f32, axis=-1, keepdims=True) / D_MODEL - row_mean * row_mean
        z_norm = ((x_f32 - row_mean) * lax.rsqrt(row_var + LN_EPS) * ln_gamma).astype(jnp.bfloat16)
        hidden = jnp.dot(z_norm, w_in, preferred_element_type=jnp.float32)
        hidden = jax.nn.gelu(hidden, approximate=True).astype(jnp.bfloat16)
        branch = jnp.dot(hidden, w_out, preferred_element_type=jnp.float32)
        return (x_f32 + branch).astype(jnp.bfloat16)

    return lax.map(one_block, row_blocks).reshape(2, MB_TOKENS, D_MODEL)
```

```python
import jax
import jax.numpy as jnp
from jax import lax
from jax.sharding import PartitionSpec as P

LN_EPS = 1e-5
CHUNKS = 8
SWAP = [(0, 1), (1, 0)]


def solution(mesh):
    col_size = mesh.shape["col"]
    act_spec = P(None, ("dp", "row"), "col")

    def per_device(x_blk, gamma_blk, w_in_blk, w_out_blk):
        n_mb, tokens, d_half = x_blk.shape
        d_model = d_half * col_size
        rows = w_out_blk.shape[0]
        n = rows // CHUNKS
        halves = w_in_blk.shape[1] // rows
        my_col = lax.axis_index("col")
        low = my_col == 0

        gamma_far = lax.ppermute(gamma_blk, "col", SWAP)
        x_far = [lax.ppermute(x_blk[m], "col", SWAP) for m in range(n_mb)]
        w_in_panels = []
        w_out_panels = []
        for c in range(CHUNKS):
            piece = jnp.concatenate([w_in_blk[:, k * rows + c * n:k * rows + (c + 1) * n] for k in range(halves)], axis=1)
            w_in_panels.append(lax.all_gather(piece, "row", axis=0, tiled=True))
        for c in range(CHUNKS):
            w_out_panels.append(lax.all_gather(w_out_blk[c * n:(c + 1) * n], "row", axis=0, tiled=True))

        z = []
        for m in range(n_mb):
            near = x_blk[m].astype(jnp.float32)
            far = x_far[m].astype(jnp.float32)
            mean = (jnp.sum(near, axis=-1) + jnp.sum(far, axis=-1)) / d_model
            var = (jnp.sum(near * near, axis=-1) + jnp.sum(far * far, axis=-1)) / d_model - mean * mean
            inv_std = lax.rsqrt(var + LN_EPS)
            z_near = ((near - mean[:, None]) * inv_std[:, None] * gamma_blk).astype(jnp.bfloat16)
            z_far = ((far - mean[:, None]) * inv_std[:, None] * gamma_far).astype(jnp.bfloat16)
            z.append(jnp.concatenate([jnp.where(low, z_near, z_far), jnp.where(low, z_far, z_near)], axis=-1))

        hid_near = [[None] * CHUNKS for _ in range(n_mb)]
        hid_far = [[None] * CHUNKS for _ in range(n_mb)]
        for c in range(CHUNKS):
            for m in range(n_mb):
                u = jnp.dot(z[m], w_in_panels[c], preferred_element_type=jnp.float32)
                h = jax.nn.gelu(u, approximate=True).astype(jnp.bfloat16)
                hid_near[m][c] = h
                hid_far[m][c] = lax.ppermute(h, "col", SWAP)

        acc = [x_blk[m].astype(jnp.float32) for m in range(n_mb)]
        branch = [None] * n_mb
        for c in range(CHUNKS):
            w_panel = w_out_panels[c]
            if c:
                *branch, w_panel = lax.optimization_barrier((*branch, w_panel))
            w = w_panel.reshape(col_size, halves * n, d_half)
            w_near = lax.dynamic_index_in_dim(w, my_col, 0, keepdims=False)
            w_far = lax.dynamic_index_in_dim(w, 1 - my_col, 0, keepdims=False)
            for m in range(n_mb):
                t = jnp.dot(hid_near[m][c], w_near, preferred_element_type=jnp.float32)
                branch[m] = t if c == 0 else branch[m] + t
                branch[m] = branch[m] + jnp.dot(hid_far[m][c], w_far, preferred_element_type=jnp.float32)
        return jnp.stack([(acc[m] + branch[m]).astype(jnp.bfloat16) for m in range(n_mb)])

    return jax.shard_map(per_device, mesh=mesh, in_specs=(act_spec, P("col"), P("row", "col"), P("row", "col")), out_specs=act_spec, check_vma=False)
```

```python
import functools
import math

import jax
import jax.numpy as jnp
from jax import lax
from jax.experimental import pallas as pl
from jax.experimental.pallas import tpu as pltpu
from jax.sharding import PartitionSpec as P

LN_EPS = 1e-5
MESH = pl.DeviceIdType.MESH
TN = 512
WINDOW = 8
EARLY = 8
TM = 256
GELU_C = math.sqrt(2 / math.pi)


def kernel(dims, x, g, w1, w2, y_out, xr, gr, w1_all, w2_all, hall,
           z, wt, hout, ln_a, ln_b, gv, acc, ht, w2t,
           xs, xrs, gs, xs1, xr1, ss1, sr1, fs1, fr1, xs2, xr2, ss2, sr2, fs2, fr2, hs, hr,
           lsem, csem, osem):
    n_mb, tok, dh, d4, hid, r4 = dims
    d_model = 2 * dh
    n1 = hid // TN
    n2 = r4 // TN
    col = lax.axis_index("col")
    row = lax.axis_index("row")
    far = 1 - col
    sib = row + 1 - 2 * lax.rem(row, 2)
    xn = lax.rem(row + 2, 4)
    xs_row = lax.rem(sib + 2, 4)
    to_col, to_x, to_sib = {"col": far}, {"row": xn}, {"row": sib}

    def remote(src, dst, ssem, rsem, dev):
        return pltpu.make_async_remote_copy(src_ref=src, dst_ref=dst, send_sem=ssem, recv_sem=rsem, device_id=dev, device_id_type=MESH)

    def cols(s):
        return pl.ds(pl.multiple_of(lax.rem(s, 2) * r4 + (s // 2) * TN, TN), TN)

    def rows2(c):
        return pl.ds(pl.multiple_of(c * TN, TN), TN)

    def x_move(m):
        return remote(x.at[m], xr.at[m], xs.at[m], xrs.at[m], to_col)

    def g_move():
        return remote(g, gr, gs.at[0], gs.at[1], to_col)

    def w1_x(s):
        return remote(w1.at[:, cols(s)], w1_all.at[row, :, cols(s)], xs1.at[s], xr1.at[s], to_x)

    def w1_sib(s):
        return remote(w1.at[:, cols(s)], w1_all.at[row, :, cols(s)], ss1.at[s], sr1.at[s], to_sib)

    def w1_fwd(s):
        return remote(w1_all.at[xn, :, cols(s)], w1_all.at[xn, :, cols(s)], fs1.at[s], fr1.at[s], to_sib)

    def w2_x(c):
        return remote(w2.at[rows2(c)], w2_all.at[row, rows2(c)], xs2.at[c], xr2.at[c], to_x)

    def w2_sib(c):
        return remote(w2.at[rows2(c)], w2_all.at[row, rows2(c)], ss2.at[c], sr2.at[c], to_sib)

    def w2_fwd(c):
        return remote(w2_all.at[xn, rows2(c)], w2_all.at[xn, rows2(c)], fs2.at[c], fr2.at[c], to_sib)

    def h_move(m, s):
        return remote(hall.at[col, m, :, cols(s)], hall.at[col, m, :, cols(s)], hs.at[m * n1 + s], hr.at[m * n1 + s], to_col)

    barrier = pltpu.get_barrier_semaphore()
    for dev in (to_col, to_x, to_sib):
        pl.semaphore_signal(barrier, inc=1, device_id=dev, device_id_type=MESH)
    pl.semaphore_wait(barrier, 3)

    g_move().start()
    for m in range(n_mb):
        x_move(m).start()

    def first_pieces(s, carry):
        w1_x(s).start()
        w1_sib(s).start()
        return carry

    lax.fori_loop(0, WINDOW, first_pieces, 0)

    def issue_after(s):
        @pl.when(s + WINDOW < n1)
        def _():
            w1_x(s + WINDOW).start()
            w1_sib(s + WINDOW).start()

        @pl.when(s + WINDOW >= n1)
        def _():
            w2_x(s + WINDOW - n1).start()
            w2_sib(s + WINDOW - n1).start()

    def layer_norm(m):
        x_move(m).wait_recv()

        def tile(t, carry):
            sl = pl.ds(pl.multiple_of(t * TM, TM), TM)
            near = pltpu.make_async_copy(x.at[m, sl], ln_a, lsem.at[0])
            other = pltpu.make_async_copy(xr.at[m, sl], ln_b, lsem.at[1])
            near.start()
            other.start()
            near.wait()
            other.wait()

            def strip(i, carry):
                rs = pl.ds(pl.multiple_of(i * 16, 16), 16)
                a = ln_a[rs, :].astype(jnp.float32)
                b = ln_b[rs, :].astype(jnp.float32)
                mean = (jnp.sum(a, axis=-1, keepdims=True) + jnp.sum(b, axis=-1, keepdims=True)) / d_model
                var = (jnp.sum(a * a, axis=-1, keepdims=True) + jnp.sum(b * b, axis=-1, keepdims=True)) / d_model - mean * mean
                inv = lax.rsqrt(var + LN_EPS)
                zr = pl.ds(pl.multiple_of(m * tok + t * TM + i * 16, 16), 16)
                z[zr, pl.ds(pl.multiple_of(col * dh, 128), dh)] = ((a - mean) * inv * gv[0:1, :]).astype(jnp.bfloat16)
                z[zr, pl.ds(pl.multiple_of(far * dh, 128), dh)] = ((b - mean) * inv * gv[1:2, :]).astype(jnp.bfloat16)
                return carry

            lax.fori_loop(0, TM // 16, strip, 0)
            return carry

        lax.fori_loop(0, tok // TM, tile, 0)

    def take_piece(s):
        w1_x(s).wait_recv()
        w1_fwd(s).start()
        issue_after(s)
        w1_sib(s).wait_recv()
        w1_fwd(s).wait_recv()

    def load_wt(s):
        copies = [pltpu.make_async_copy(w1.at[:, cols(s)], wt.at[pl.ds(pl.multiple_of(row * d4, d4), d4)], lsem.at[0])]
        for j, b in enumerate((sib, xn, xs_row)):
            copies.append(pltpu.make_async_copy(w1_all.at[b, :, cols(s)], wt.at[pl.ds(pl.multiple_of(b * d4, d4), d4)], lsem.at[j + 1]))
        for cp in copies:
            cp.start()
        for cp in copies:
            cp.wait()

    def first_product(m, s):
        def tile(t, carry):
            rs = pl.ds(pl.multiple_of(t * TM, TM), TM)
            zr = pl.ds(pl.multiple_of(m * tok + t * TM, TM), TM)
            u = jnp.dot(z[zr, :], wt[...], preferred_element_type=jnp.float32)
            h = 0.5 * u * (1.0 + jnp.tanh(GELU_C * (u + 0.044715 * (u * u * u))))
            hout[rs, :] = h.astype(jnp.bfloat16)
            return carry

        lax.fori_loop(0, tok // TM, tile, 0)
        cp = pltpu.make_async_copy(hout, hall.at[col, m, :, cols(s)], csem.at[0])
        cp.start()
        cp.wait()
        h_move(m, s).start()

    g_move().wait_recv()
    for i, src in enumerate((g, gr)):
        cp = pltpu.make_async_copy(src, gv.at[pl.ds(i, 1)], lsem.at[0])
        cp.start()
        cp.wait()
    layer_norm(0)

    def early_a(s, carry):
        take_piece(s)
        load_wt(s)
        first_product(0, s)
        return carry

    def early_b(s, carry):
        load_wt(s)
        first_product(1, s)
        return carry

    def rest(s, carry):
        take_piece(s)
        load_wt(s)

        def each(m, carry):
            first_product(m, s)
            return carry

        lax.fori_loop(0, n_mb, each, 0)
        return carry

    lax.fori_loop(0, EARLY, early_a, 0)
    layer_norm(1)
    lax.fori_loop(0, EARLY, early_b, 0)
    lax.fori_loop(EARLY, n1, rest, 0)

    def init(t, carry):
        m, q = t // (tok // TM), lax.rem(t, tok // TM)
        cp = pltpu.make_async_copy(x.at[m, pl.ds(pl.multiple_of(q * TM, TM), TM)], ln_a, lsem.at[0])
        cp.start()
        cp.wait()
        acc[pl.ds(pl.multiple_of(t * TM, TM), TM), :] = ln_a[...].astype(jnp.float32)
        return carry

    lax.fori_loop(0, n_mb * tok // TM, init, 0)

    def chunk(c, last):
        for m in range(n_mb):
            for k in range(2):
                h_move(m, 2 * c + k).wait_recv()
        w2_sib(c).wait_recv()
        blocks = (row, sib, xn, xs_row)

        def load(j):
            b, slot = blocks[j], j % 2
            hc = pl.ds(pl.multiple_of(lax.rem(b, 2) * r4 + c * TN, TN), TN)
            src = w2.at[rows2(c)] if j == 0 else w2_all.at[b, rows2(c)]
            return [pltpu.make_async_copy(src, w2t.at[slot], lsem.at[2 * slot])] + [
                pltpu.make_async_copy(hall.at[b // 2, m, :, hc], ht.at[slot, pl.ds(m * tok, tok)], csem.at[n_mb * slot + m]) for m in range(n_mb)]

        def start(j):
            for cp in load(j):
                cp.start()

        def wait(j):
            for cp in load(j):
                cp.wait()

        def product(j, drain):
            slot = j % 2

            def tile(t, carry):
                rs = pl.ds(pl.multiple_of(t * TM, TM), TM)

                def part(i, carry):
                    cs = pl.ds(pl.multiple_of(i * TN, TN), TN)
                    acc[rs, cs] += jnp.dot(ht[slot, rs, :], w2t[slot, :, cs], preferred_element_type=jnp.float32)
                    return carry

                lax.fori_loop(0, dh // TN, part, 0)
                if drain:
                    drain(t, rs)
                return carry

            lax.fori_loop(0, n_mb * tok // TM, tile, 0)

        start(0)
        start(1)
        wait(0)
        product(0, None)
        w2_x(c).wait_recv()
        w2_fwd(c).start()
        if not last:
            @pl.when(c + WINDOW < n2)
            def _():
                w2_x(c + WINDOW).start()
                w2_sib(c + WINDOW).start()
        start(2)
        wait(1)
        product(1, None)
        w2_fwd(c).wait_recv()
        start(3)
        wait(2)
        product(2, None)
        wait(3)
        if not last:
            product(3, None)
            return

        def out_copy(t, buf, sem):
            m, q = t // (tok // TM), lax.rem(t, tok // TM)
            return pltpu.make_async_copy(buf, y_out.at[m, pl.ds(pl.multiple_of(q * TM, TM), TM)], sem)

        def drain(t, rs):
            for p, buf in enumerate((ln_a, ln_b)):
                @pl.when(lax.rem(t, 2) == p)
                def _():
                    @pl.when(t >= 2)
                    def _():
                        out_copy(t - 2, buf, osem.at[p]).wait()
                    buf[...] = acc[rs, :].astype(jnp.bfloat16)
                    out_copy(t, buf, osem.at[p]).start()

        product(3, drain)
        steps = n_mb * tok // TM
        for p, buf in enumerate((ln_a, ln_b)):
            out_copy(steps - 2 + p, buf, osem.at[p]).wait()

    def middle(c, carry):
        chunk(c, False)
        return carry

    lax.fori_loop(0, n2 - 1, middle, 0)
    chunk(n2 - 1, True)

    g_move().wait_send()
    for m in range(n_mb):
        x_move(m).wait_send()

    def sent1(s, carry):
        w1_x(s).wait_send()
        w1_sib(s).wait_send()
        w1_fwd(s).wait_send()
        for m in range(n_mb):
            h_move(m, s).wait_send()
        return carry

    def sent2(c, carry):
        w2_x(c).wait_send()
        w2_sib(c).wait_send()
        w2_fwd(c).wait_send()
        return carry

    lax.fori_loop(0, n1, sent1, 0)
    lax.fori_loop(0, n2, sent2, 0)


def solution(mesh):
    act_spec = P(None, ("dp", "row"), "col")

    def per_device(x, gamma, w1, w2):
        n_mb, tok, dh = x.shape
        d4, hid = w1.shape
        r4 = w2.shape[0]
        n1, n2 = hid // TN, r4 // TN
        bf16, f32 = jnp.bfloat16, jnp.float32
        dma = pltpu.SemaphoreType.DMA
        any_spec = pl.BlockSpec(memory_space=pl.ANY)
        shapes = (
            jax.ShapeDtypeStruct((n_mb, tok, dh), bf16),
            jax.ShapeDtypeStruct((n_mb, tok, dh), bf16),
            jax.ShapeDtypeStruct((1, dh), f32),
            jax.ShapeDtypeStruct((4, d4, hid), bf16),
            jax.ShapeDtypeStruct((4, r4, dh), bf16),
            jax.ShapeDtypeStruct((2, n_mb, tok, hid), bf16),
        )
        outs = pl.pallas_call(
            functools.partial(kernel, (n_mb, tok, dh, d4, hid, r4)),
            out_shape=shapes,
            in_specs=[any_spec] * 4,
            out_specs=[any_spec] * len(shapes),
            scratch_shapes=[
                pltpu.VMEM((n_mb * tok, 2 * dh), bf16),
                pltpu.VMEM((4 * d4, TN), bf16),
                pltpu.VMEM((tok, TN), bf16),
                pltpu.VMEM((TM, dh), bf16),
                pltpu.VMEM((TM, dh), bf16),
                pltpu.VMEM((2, dh), f32),
                pltpu.VMEM((n_mb * tok, dh), f32),
                pltpu.VMEM((2, n_mb * tok, TN), bf16),
                pltpu.VMEM((2, TN, dh), bf16),
                dma((n_mb,)), dma((n_mb,)), dma((2,)),
                dma((n1,)), dma((n1,)), dma((n1,)), dma((n1,)), dma((n1,)), dma((n1,)),
                dma((n2,)), dma((n2,)), dma((n2,)), dma((n2,)), dma((n2,)), dma((n2,)),
                dma((n_mb * n1,)), dma((n_mb * n1,)),
                dma((4,)), dma((4,)), dma((2,)),
            ],
            compiler_params=pltpu.CompilerParams(collective_id=0, has_side_effects=True, vmem_limit_bytes=67043328),
        )(x, gamma.reshape(1, dh), w1, w2)
        return outs[0]

    return jax.shard_map(per_device, mesh=mesh, in_specs=(act_spec, P("col"), P("row", "col"), P("row", "col")), out_specs=act_spec, check_vma=False)
```

```python
import functools
import math

import jax
import jax.numpy as jnp
from jax import lax
from jax.experimental import pallas as pl
from jax.experimental.pallas import tpu as pltpu
from jax.sharding import PartitionSpec as P

LN_EPS = 1e-5
MESH = pl.DeviceIdType.MESH
TN = 512
WINDOW = 8
EARLY = 8
TM = 256
SUB = 256
GELU_C = math.sqrt(2 / math.pi)


def kernel(dims, x, g, w1, w2, y_out, xr, gr, w1_all, w2_all, hall,
           z, wt, hout, ln_a, ln_b, gv, acc,
           xs, xrs, gs, xs1, xr1, ss1, sr1, fs1, fr1, xs2, xr2, ss2, sr2, fs2, fr2, hs, hr,
           lsem, csem, osem, wsem):
    n_mb, tok, dh, d4, hid, r4 = dims
    d_model = 2 * dh
    n1 = hid // TN
    n2 = r4 // TN
    n_sub = TN // SUB
    col = lax.axis_index("col")
    row = lax.axis_index("row")
    far = 1 - col
    sib = row + 1 - 2 * lax.rem(row, 2)
    xn = lax.rem(row + 2, 4)
    xs_row = lax.rem(sib + 2, 4)
    to_col, to_x, to_sib = {"col": far}, {"row": xn}, {"row": sib}

    def remote(src, dst, ssem, rsem, dev):
        return pltpu.make_async_remote_copy(src_ref=src, dst_ref=dst, send_sem=ssem, recv_sem=rsem, device_id=dev, device_id_type=MESH)

    def cols(s):
        return pl.ds(pl.multiple_of(lax.rem(s, 2) * r4 + (s // 2) * TN, TN), TN)

    def rows2(p):
        if isinstance(p, int) and p >= n2 - 1:
            return pl.ds((n2 - 1) * TN + (p - n2 + 1) * SUB, SUB)
        return pl.ds(pl.multiple_of(p * TN, TN), TN)

    def x_move(m):
        return remote(x.at[m], xr.at[m], xs.at[m], xrs.at[m], to_col)

    def g_move():
        return remote(g, gr, gs.at[0], gs.at[1], to_col)

    def w1_x(s):
        return remote(w1.at[:, cols(s)], w1_all.at[row, s], xs1.at[s], xr1.at[s], to_x)

    def w1_sib(s):
        return remote(w1.at[:, cols(s)], w1_all.at[row, s], ss1.at[s], sr1.at[s], to_sib)

    def w1_fwd(s):
        return remote(w1_all.at[xn, s], w1_all.at[xn, s], fs1.at[s], fr1.at[s], to_sib)

    def w2_x(c):
        return remote(w2.at[rows2(c)], w2_all.at[row, rows2(c)], xs2.at[c], xr2.at[c], to_x)

    def w2_sib(c):
        return remote(w2.at[rows2(c)], w2_all.at[row, rows2(c)], ss2.at[c], sr2.at[c], to_sib)

    def w2_fwd(c):
        return remote(w2_all.at[xn, rows2(c)], w2_all.at[xn, rows2(c)], fs2.at[c], fr2.at[c], to_sib)

    def h_early(m, s):
        q = m * EARLY + s
        return remote(hall.at[col, s, m], hall.at[col, s, m], hs.at[q], hr.at[q], to_col)

    def h_pair(s):
        q = (n_mb - 1) * EARLY + s
        return remote(hall.at[col, s], hall.at[col, s], hs.at[q], hr.at[q], to_col)

    def h_last(k, u):
        s = n1 - 2 + k
        q = (n_mb - 1) * EARLY + n1 - 2 + k * n_sub + u
        return remote(hall.at[col, s, :, u], hall.at[col, s, :, u], hs.at[q], hr.at[q], to_col)

    barrier = pltpu.get_barrier_semaphore()
    for dev in (to_col, to_x, to_sib):
        pl.semaphore_signal(barrier, inc=1, device_id=dev, device_id_type=MESH)
    pl.semaphore_wait(barrier, 3)

    g_move().start()
    for m in range(n_mb):
        x_move(m).start()

    def first_pieces(s, carry):
        w1_x(s).start()
        w1_sib(s).start()
        return carry

    lax.fori_loop(0, WINDOW, first_pieces, 0)

    def issue_after(s):
        @pl.when(s + WINDOW < n1)
        def _():
            w1_x(s + WINDOW).start()
            w1_sib(s + WINDOW).start()

        @pl.when(s + WINDOW >= n1)
        def _():
            w2_x(s + WINDOW - n1).start()
            w2_sib(s + WINDOW - n1).start()

    def layer_norm(m):
        x_move(m).wait_recv()

        ga = gv[0:1, :]
        gb = gv[1:2, :]

        def tile(t, carry):
            sl = pl.ds(pl.multiple_of(t * TM, TM), TM)
            near = pltpu.make_async_copy(x.at[m, sl], ln_a, lsem.at[0])
            other = pltpu.make_async_copy(xr.at[m, sl], ln_b, lsem.at[1])
            near.start()
            other.start()
            near.wait()
            other.wait()

            def strip(i, carry):
                rs = pl.ds(pl.multiple_of(i * 16, 16), 16)
                a = ln_a[rs, :].astype(jnp.float32)
                b = ln_b[rs, :].astype(jnp.float32)
                mean = (jnp.sum(a, axis=-1, keepdims=True) + jnp.sum(b, axis=-1, keepdims=True)) / d_model
                var = (jnp.sum(a * a, axis=-1, keepdims=True) + jnp.sum(b * b, axis=-1, keepdims=True)) / d_model - mean * mean
                inv = lax.rsqrt(var + LN_EPS)
                zr = pl.ds(pl.multiple_of(m * tok + t * TM + i * 16, 16), 16)
                z[zr, pl.ds(pl.multiple_of(col * dh, 128), dh)] = ((a - mean) * inv * ga).astype(jnp.bfloat16)
                z[zr, pl.ds(pl.multiple_of(far * dh, 128), dh)] = ((b - mean) * inv * gb).astype(jnp.bfloat16)
                return carry

            lax.fori_loop(0, TM // 16, strip, 0)
            return carry

        lax.fori_loop(0, tok // TM, tile, 0)

    def take_piece(s):
        w1_x(s).wait_recv()
        w1_fwd(s).start()
        issue_after(s)
        w1_sib(s).wait_recv()
        w1_fwd(s).wait_recv()

    def wt_copies(s):
        base = lax.rem(s, 2) * (4 * d4)
        sem0 = 4 * lax.rem(s, 2)

        def rows(b):
            return wt.at[pl.ds(pl.multiple_of(base + b * d4, d4), d4)]

        copies = [pltpu.make_async_copy(w1.at[:, cols(s)], rows(row), lsem.at[sem0])]
        for j, b in enumerate((sib, xn, xs_row)):
            copies.append(pltpu.make_async_copy(w1_all.at[b, s], rows(b), lsem.at[sem0 + j + 1]))
        return copies

    def load_wt(s):
        for cp in wt_copies(s):
            cp.start()

    def wait_wt(s):
        for cp in wt_copies(s):
            cp.wait()

    def first_product(m, s):
        base = pl.multiple_of(lax.rem(s, 2) * (4 * d4), 4 * d4)

        def tile(t, carry):
            rs = pl.ds(pl.multiple_of(t * TM, TM), TM)
            zr = pl.ds(pl.multiple_of(m * tok + t * TM, TM), TM)
            u = jnp.dot(z[zr, :], wt[pl.ds(base, 4 * d4), :], preferred_element_type=jnp.float32)
            h = 0.5 * u * (1.0 + jnp.tanh(GELU_C * (u + 0.044715 * (u * u * u))))
            hout[rs, :] = h.astype(jnp.bfloat16)
            return carry

        lax.fori_loop(0, tok // TM, tile, 0)
        copies = [pltpu.make_async_copy(hout.at[:, u * SUB:(u + 1) * SUB], hall.at[col, s, m, u], csem.at[u]) for u in range(n_sub)]
        for cp in copies:
            cp.start()
        for cp in copies:
            cp.wait()

    g_move().wait_recv()
    for i, src in enumerate((g, gr)):
        cp = pltpu.make_async_copy(src, gv.at[pl.ds(i, 1)], lsem.at[0])
        cp.start()
        cp.wait()
    layer_norm(0)

    def early_a(s, carry):
        take_piece(s)
        load_wt(s)
        wait_wt(s)
        first_product(0, s)
        h_early(0, s).start()
        return carry

    def early_b(s, carry):
        wait_wt(s)

        @pl.when(s + 1 < EARLY)
        def _():
            load_wt(s + 1)

        first_product(1, s)
        h_early(1, s).start()
        return carry

    def both(s):
        take_piece(s)
        load_wt(s)
        wait_wt(s)

        def each(m, carry):
            first_product(m, s)
            return carry

        lax.fori_loop(0, n_mb, each, 0)

    def rest(s, carry):
        both(s)

        @pl.when(s < n1 - 2)
        def _():
            h_pair(s).start()

        return carry

    lax.fori_loop(0, EARLY, early_a, 0)
    layer_norm(1)
    load_wt(0)
    lax.fori_loop(0, EARLY, early_b, 0)
    lax.fori_loop(EARLY, n1, rest, 0)
    for u in range(n_sub):
        for k in range(2):
            h_last(k, u).start()

    def init(t, carry):
        m, q = t // (tok // TM), lax.rem(t, tok // TM)
        cp = pltpu.make_async_copy(x.at[m, pl.ds(pl.multiple_of(q * TM, TM), TM)], ln_a, lsem.at[0])
        cp.start()
        cp.wait()
        acc[pl.ds(pl.multiple_of(t * TM, TM), TM), :] = ln_a[...].astype(jnp.float32)
        return carry

    lax.fori_loop(0, n_mb * tok // TM, init, 0)

    def h_copies(c, u, g):
        size = TN if u is None else SUB
        subs = range(n_sub) if u is None else (u,)
        half = row // 2 if g == 0 else 1 - row // 2
        copies = []
        for k in range(2):
            for m in range(n_mb):
                for q, v in enumerate(subs):
                    dst = z.at[pl.ds(m * tok, tok), pl.ds(g * 2 * TN + k * size + q * SUB, SUB)]
                    copies.append(pltpu.make_async_copy(hall.at[half, 2 * c + k, m, v], dst, csem.at[len(copies) + 8 * g]))
        return copies

    def w2_copies(p, size, g, src_own, b, lane):
        k = lax.rem(b, 2)
        copies = []
        for i in range(dh // TN):
            rows = pl.ds(pl.multiple_of(g * (dh // TN) * 2 * TN + i * 2 * size + k * size, SUB), size)
            src = (w2.at[rows2(p)] if src_own else w2_all.at[b, rows2(p)]).at[:, i * TN:(i + 1) * TN]
            copies.append(pltpu.make_async_copy(src, wt.at[rows], wsem.at[lane * (dh // TN) + i]))
        return copies

    def product(size, g, drain):
        base = g * (dh // TN) * 2 * TN

        def tile(t, carry):
            rs = pl.ds(pl.multiple_of(t * TM, TM), TM)

            def part(i, carry):
                cs = pl.ds(pl.multiple_of(i * TN, TN), TN)
                ws = pl.ds(pl.multiple_of(base + i * 2 * size, SUB), 2 * size)
                acc[rs, cs] += jnp.dot(z[rs, g * 2 * TN:g * 2 * TN + 2 * size], wt[ws, :], preferred_element_type=jnp.float32)
                return carry

            lax.fori_loop(0, dh // TN, part, 0)
            if drain:
                drain(t, rs)
            return carry

        lax.fori_loop(0, n_mb * tok // TM, tile, 0)

    def out_copy(t, buf, sem):
        m, q = t // (tok // TM), lax.rem(t, tok // TM)
        return pltpu.make_async_copy(buf, y_out.at[m, pl.ds(pl.multiple_of(q * TM, TM), TM)], sem)

    def drain_tile(t, rs):
        for p, buf in enumerate((ln_a, ln_b)):
            @pl.when(lax.rem(t, 2) == p)
            def _():
                @pl.when(t >= 2)
                def _():
                    out_copy(t - 2, buf, osem.at[p]).wait()
                buf[...] = acc[rs, :].astype(jnp.bfloat16)
                out_copy(t, buf, osem.at[p]).start()

    def start(copies):
        for cp in copies:
            cp.start()

    def finish(copies):
        for cp in copies:
            cp.wait()

    def chunk(p, c, u, drain):
        size = TN if u is None else SUB
        own = w2_copies(p, size, 0, True, row, 0)
        start(own)

        def wait_h():
            if u is None:
                @pl.when(c < EARLY // 2)
                def _():
                    for m in range(n_mb):
                        for k in range(2):
                            h_early(m, 2 * c + k).wait_recv()

                @pl.when(c >= EARLY // 2)
                def _():
                    for k in range(2):
                        h_pair(2 * c + k).wait_recv()
            else:
                for k in range(2):
                    h_last(k, u).wait_recv()

        w2_sib(p).wait_recv()
        sib_w = w2_copies(p, size, 0, False, sib, 1)
        start(sib_w)

        @pl.when(row // 2 != col)
        def _():
            wait_h()

        h0 = h_copies(c, u, 0)
        h1 = h_copies(c, u, 1)
        start(h0)
        finish(own)
        finish(sib_w)
        finish(h0)
        product(size, 0, None)

        @pl.when(row // 2 == col)
        def _():
            wait_h()

        start(h1)
        w2_x(p).wait_recv()
        w2_fwd(p).start()
        if u is None:
            @pl.when(c + WINDOW < n2 - 1)
            def _():
                w2_x(c + WINDOW).start()
                w2_sib(c + WINDOW).start()
        x_w = w2_copies(p, size, 1, False, xn, 2)
        start(x_w)
        w2_fwd(p).wait_recv()
        f_w = w2_copies(p, size, 1, False, xs_row, 3)
        start(f_w)
        finish(h1)
        finish(x_w)
        finish(f_w)
        product(size, 1, drain)

    def middle(c, carry):
        chunk(c, c, None, None)

        @pl.when(c == 0)
        def _():
            for p in range(n2 - 1, n2 - 1 + n_sub):
                w2_x(p).start()
                w2_sib(p).start()

        return carry

    lax.fori_loop(0, n2 - 1, middle, 0)
    for u in range(n_sub):
        chunk(n2 - 1 + u, n2 - 1, u, drain_tile if u == n_sub - 1 else None)
    steps = n_mb * tok // TM
    for p, buf in enumerate((ln_a, ln_b)):
        out_copy(steps - 2 + p, buf, osem.at[p]).wait()

    g_move().wait_send()
    for m in range(n_mb):
        x_move(m).wait_send()

    def sent1(s, carry):
        w1_x(s).wait_send()
        w1_sib(s).wait_send()
        w1_fwd(s).wait_send()
        return carry

    def sent2(c, carry):
        w2_x(c).wait_send()
        w2_sib(c).wait_send()
        w2_fwd(c).wait_send()
        return carry

    def sent_early(s, carry):
        for m in range(n_mb):
            h_early(m, s).wait_send()
        return carry

    def sent_pair(s, carry):
        h_pair(s).wait_send()
        return carry

    lax.fori_loop(0, n1, sent1, 0)
    lax.fori_loop(0, n2 - 1, sent2, 0)
    for p in range(n2 - 1, n2 - 1 + n_sub):
        sent2(p, 0)
    lax.fori_loop(0, EARLY, sent_early, 0)
    lax.fori_loop(EARLY, n1 - 2, sent_pair, 0)
    for u in range(n_sub):
        for k in range(2):
            h_last(k, u).wait_send()


def solution(mesh):
    act_spec = P(None, ("dp", "row"), "col")

    def per_device(x, gamma, w1, w2):
        n_mb, tok, dh = x.shape
        d4, hid = w1.shape
        r4 = w2.shape[0]
        n1, n2 = hid // TN, r4 // TN
        n2p = n2 - 1 + TN // SUB
        nh = (n_mb - 1) * EARLY + n1 - 2 + 2 * (TN // SUB)
        bf16, f32 = jnp.bfloat16, jnp.float32
        dma = pltpu.SemaphoreType.DMA
        any_spec = pl.BlockSpec(memory_space=pl.ANY)
        shapes = (
            jax.ShapeDtypeStruct((n_mb, tok, dh), bf16),
            jax.ShapeDtypeStruct((n_mb, tok, dh), bf16),
            jax.ShapeDtypeStruct((1, dh), f32),
            jax.ShapeDtypeStruct((4, n1, d4, TN), bf16),
            jax.ShapeDtypeStruct((4, r4, dh), bf16),
            jax.ShapeDtypeStruct((2, n1, n_mb, TN // SUB, tok, SUB), bf16),
        )
        outs = pl.pallas_call(
            functools.partial(kernel, (n_mb, tok, dh, d4, hid, r4)),
            out_shape=shapes,
            in_specs=[any_spec] * 4,
            out_specs=[any_spec] * len(shapes),
            scratch_shapes=[
                pltpu.VMEM((n_mb * tok, 2 * dh), bf16),
                pltpu.VMEM((8 * d4, TN), bf16),
                pltpu.VMEM((tok, TN), bf16),
                pltpu.VMEM((TM, dh), bf16),
                pltpu.VMEM((TM, dh), bf16),
                pltpu.VMEM((2, dh), f32),
                pltpu.VMEM((n_mb * tok, dh), f32),
                dma((n_mb,)), dma((n_mb,)), dma((2,)),
                dma((n1,)), dma((n1,)), dma((n1,)), dma((n1,)), dma((n1,)), dma((n1,)),
                dma((n2p,)), dma((n2p,)), dma((n2p,)), dma((n2p,)), dma((n2p,)), dma((n2p,)),
                dma((nh,)), dma((nh,)),
                dma((8,)), dma((16,)), dma((2,)), dma((4 * (dh // TN),)),
            ],
            compiler_params=pltpu.CompilerParams(collective_id=0, has_side_effects=True, vmem_limit_bytes=67043328),
        )(x, gamma.reshape(1, dh), w1, w2)
        return outs[0]

    return jax.shard_map(per_device, mesh=mesh, in_specs=(act_spec, P("col"), P("row", "col"), P("row", "col")), out_specs=act_spec, check_vma=False)
```

```python
import functools
import math

import jax
import jax.numpy as jnp
from jax import lax
from jax.experimental import pallas as pl
from jax.experimental.pallas import tpu as pltpu
from jax.sharding import PartitionSpec as P

LN_EPS = 1e-5
MESH = pl.DeviceIdType.MESH
TN = 512
WINDOW = 8
EARLY = 8
TM = 256
SUB = 128
LAST = (256, 128, 128)
GELU_C = math.sqrt(2 / math.pi)


def kernel(dims, x, g, w1, w2, y_out, xr, gr, w1_all, w2_all, hall,
           z, wt, hout, ln_a, ln_b, g_rows, gv, acc,
           xs, xrs, gs, xs1, xr1, ss1, sr1, fs1, fr1, xs2, xr2, ss2, sr2, fs2, fr2, hs, hr,
           lsem, csem, osem, wsem):
    n_mb, tok, dh, d4, hid, r4 = dims
    d_model = 2 * dh
    n1 = hid // TN
    n2 = r4 // TN
    n_sub = TN // SUB
    last_at = [sum(LAST[:u]) for u in range(len(LAST))]
    col = lax.axis_index("col")
    row = lax.axis_index("row")
    far = 1 - col
    sib = row + 1 - 2 * lax.rem(row, 2)
    xn = lax.rem(row + 2, 4)
    xs_row = lax.rem(sib + 2, 4)
    diagonal = row // 2 == col
    to_col, to_x, to_sib = {"col": far}, {"row": xn}, {"row": sib}

    def remote(src, dst, ssem, rsem, dev):
        return pltpu.make_async_remote_copy(src_ref=src, dst_ref=dst, send_sem=ssem, recv_sem=rsem, device_id=dev, device_id_type=MESH)

    def cols(s):
        return pl.ds(pl.multiple_of(lax.rem(s, 2) * r4 + (s // 2) * TN, TN), TN)

    def rows2(p):
        if isinstance(p, int) and p >= n2 - 1:
            return pl.ds((n2 - 1) * TN + last_at[p - n2 + 1], LAST[p - n2 + 1])
        return pl.ds(pl.multiple_of(p * TN, TN), TN)

    def x_move(m):
        return remote(x.at[m], xr.at[m], xs.at[m], xrs.at[m], to_col)

    def g_move():
        return remote(g, gr, gs.at[0], gs.at[1], to_col)

    def w1_x(s):
        return remote(w1.at[:, cols(s)], w1_all.at[row, s], xs1.at[s], xr1.at[s], to_x)

    def w1_sib(s):
        return remote(w1.at[:, cols(s)], w1_all.at[row, s], ss1.at[s], sr1.at[s], to_sib)

    def w1_fwd(s):
        return remote(w1_all.at[xn, s], w1_all.at[xn, s], fs1.at[s], fr1.at[s], to_sib)

    def w2_x(c):
        return remote(w2.at[rows2(c)], w2_all.at[row, rows2(c)], xs2.at[c], xr2.at[c], to_x)

    def w2_sib(c):
        return remote(w2.at[rows2(c)], w2_all.at[row, rows2(c)], ss2.at[c], sr2.at[c], to_sib)

    def w2_fwd(c):
        return remote(w2_all.at[xn, rows2(c)], w2_all.at[xn, rows2(c)], fs2.at[c], fr2.at[c], to_sib)

    def h_early(m, s):
        q = m * EARLY + s
        return remote(hall.at[col, s, m], hall.at[col, s, m], hs.at[q], hr.at[q], to_col)

    def h_pair(s):
        q = (n_mb - 1) * EARLY + s
        return remote(hall.at[col, s], hall.at[col, s], hs.at[q], hr.at[q], to_col)

    def h_last(k, u):
        s = n1 - 2 + k
        q = (n_mb - 1) * EARLY + n1 - 2 + k * len(LAST) + u
        subs = pl.ds(last_at[u] // SUB, LAST[u] // SUB)
        return remote(hall.at[col, s, :, subs], hall.at[col, s, :, subs], hs.at[q], hr.at[q], to_col)

    barrier = pltpu.get_barrier_semaphore()
    for dev in (to_col, to_x, to_sib):
        pl.semaphore_signal(barrier, inc=1, device_id=dev, device_id_type=MESH)
    pl.semaphore_wait(barrier, 3)

    g_move().start()
    for m in range(n_mb):
        x_move(m).start()

    def first_pieces(s, carry):
        w1_x(s).start()
        w1_sib(s).start()
        return carry

    lax.fori_loop(0, WINDOW, first_pieces, 0)

    def issue_after(s):
        @pl.when(s + WINDOW < n1)
        def _():
            w1_x(s + WINDOW).start()
            w1_sib(s + WINDOW).start()

        @pl.when(s + WINDOW >= n1)
        def _():
            w2_x(s + WINDOW - n1).start()
            w2_sib(s + WINDOW - n1).start()

    def layer_norm(m):
        x_move(m).wait_recv()

        ga = gv[0:1, :]
        gb = gv[1:2, :]

        def tile(t, carry):
            sl = pl.ds(pl.multiple_of(t * TM, TM), TM)
            near = pltpu.make_async_copy(x.at[m, sl], ln_a, lsem.at[0])
            other = pltpu.make_async_copy(xr.at[m, sl], ln_b, lsem.at[1])
            near.start()
            other.start()
            near.wait()
            other.wait()

            def strip(i, carry):
                rs = pl.ds(pl.multiple_of(i * 16, 16), 16)
                a = ln_a[rs, :].astype(jnp.float32)
                b = ln_b[rs, :].astype(jnp.float32)
                mean = (jnp.sum(a, axis=-1, keepdims=True) + jnp.sum(b, axis=-1, keepdims=True)) / d_model
                var = (jnp.sum(a * a, axis=-1, keepdims=True) + jnp.sum(b * b, axis=-1, keepdims=True)) / d_model - mean * mean
                inv = lax.rsqrt(var + LN_EPS)
                zr = pl.ds(pl.multiple_of(m * tok + t * TM + i * 16, 16), 16)
                z[zr, pl.ds(pl.multiple_of(col * dh, 128), dh)] = ((a - mean) * inv * ga).astype(jnp.bfloat16)
                z[zr, pl.ds(pl.multiple_of(far * dh, 128), dh)] = ((b - mean) * inv * gb).astype(jnp.bfloat16)
                return carry

            lax.fori_loop(0, TM // 16, strip, 0)
            return carry

        lax.fori_loop(0, tok // TM, tile, 0)

    def take_piece(s):
        w1_x(s).wait_recv()
        w1_fwd(s).start()
        issue_after(s)
        w1_sib(s).wait_recv()
        w1_fwd(s).wait_recv()

    def wt_copies(s):
        base = lax.rem(s, 2) * (4 * d4)
        sem0 = 4 * lax.rem(s, 2)

        def rows(b):
            return wt.at[pl.ds(pl.multiple_of(base + b * d4, d4), d4)]

        copies = [pltpu.make_async_copy(w1.at[:, cols(s)], rows(row), lsem.at[sem0])]
        for j, b in enumerate((sib, xn, xs_row)):
            copies.append(pltpu.make_async_copy(w1_all.at[b, s], rows(b), lsem.at[sem0 + j + 1]))
        return copies

    def load_wt(s):
        for cp in wt_copies(s):
            cp.start()

    def wait_wt(s):
        for cp in wt_copies(s):
            cp.wait()

    def first_product(m, s):
        base = pl.multiple_of(lax.rem(s, 2) * (4 * d4), 4 * d4)

        def tile(t, carry):
            rs = pl.ds(pl.multiple_of(t * TM, TM), TM)
            zr = pl.ds(pl.multiple_of(m * tok + t * TM, TM), TM)
            u = jnp.dot(z[zr, :], wt[pl.ds(base, 4 * d4), :], preferred_element_type=jnp.float32)
            h = 0.5 * u * (1.0 + jnp.tanh(GELU_C * (u + 0.044715 * (u * u * u))))
            hout[rs, :] = h.astype(jnp.bfloat16)
            return carry

        lax.fori_loop(0, tok // TM, tile, 0)
        copies = [pltpu.make_async_copy(hout.at[:, u * SUB:(u + 1) * SUB], hall.at[col, s, m, u], csem.at[u]) for u in range(n_sub)]
        for cp in copies:
            cp.start()
        for cp in copies:
            cp.wait()

    g_move().wait_recv()
    for i, src in enumerate((g, gr)):
        cp = pltpu.make_async_copy(src, g_rows.at[i], lsem.at[0])
        cp.start()
        cp.wait()
        for j in range(dh // 128):
            gv[i:i + 1, j * 128:(j + 1) * 128] = g_rows[i, j:j + 1, :]
    layer_norm(0)

    def early_a(s, carry):
        take_piece(s)
        load_wt(s)
        wait_wt(s)
        first_product(0, s)
        h_early(0, s).start()
        return carry

    def early_b(s, carry):
        wait_wt(s)

        @pl.when(s + 1 < EARLY)
        def _():
            load_wt(s + 1)

        first_product(1, s)
        h_early(1, s).start()
        return carry

    def both(s):
        take_piece(s)
        load_wt(s)
        wait_wt(s)

        def each(m, carry):
            first_product(m, s)
            return carry

        lax.fori_loop(0, n_mb, each, 0)

    def rest(s, carry):
        both(s)

        @pl.when(s < n1 - 2)
        def _():
            h_pair(s).start()

        return carry

    lax.fori_loop(0, EARLY, early_a, 0)
    layer_norm(1)
    load_wt(0)
    lax.fori_loop(0, EARLY, early_b, 0)
    lax.fori_loop(EARLY, n1, rest, 0)
    for u in range(len(LAST)):
        for k in range(2):
            h_last(k, u).start()

    def init(t, carry):
        m, q = t // (tok // TM), lax.rem(t, tok // TM)
        cp = pltpu.make_async_copy(x.at[m, pl.ds(pl.multiple_of(q * TM, TM), TM)], ln_a, lsem.at[0])
        cp.start()
        cp.wait()
        acc[pl.ds(pl.multiple_of(t * TM, TM), TM), :] = ln_a[...].astype(jnp.float32)
        return carry

    lax.fori_loop(0, n_mb * tok // TM, init, 0)

    def h_copies(c, u, g):
        size = TN if u is None else LAST[u]
        subs = range(n_sub) if u is None else range(last_at[u] // SUB, (last_at[u] + LAST[u]) // SUB)
        half = row // 2 if g == 0 else 1 - row // 2
        copies = []
        for k in range(2):
            for m in range(n_mb):
                for q, v in enumerate(subs):
                    dst = z.at[pl.ds(m * tok, tok), pl.ds(g * 2 * TN + k * size + q * SUB, SUB)]
                    copies.append(pltpu.make_async_copy(hall.at[half, 2 * c + k, m, v], dst, csem.at[len(copies) + 4 * n_sub * g]))
        return copies

    def w2_copies(p, size, g, src_own, b, lane):
        k = lax.rem(b, 2)
        copies = []
        for i in range(dh // TN):
            rows = pl.ds(pl.multiple_of(g * (dh // TN) * 2 * TN + i * 2 * size + k * size, SUB), size)
            src = (w2.at[rows2(p)] if src_own else w2_all.at[b, rows2(p)]).at[:, i * TN:(i + 1) * TN]
            copies.append(pltpu.make_async_copy(src, wt.at[rows], wsem.at[lane * (dh // TN) + i]))
        return copies

    def product(size, g, drain=None):
        base = g * (dh // TN) * 2 * TN

        def tile(t, carry):
            rs = pl.ds(pl.multiple_of(t * TM, TM), TM)

            for i in range(dh // TN):
                cs = slice(i * TN, (i + 1) * TN)
                ws = slice(base + i * 2 * size, base + (i + 1) * 2 * size)
                acc[rs, cs] += jnp.dot(z[rs, g * 2 * TN:g * 2 * TN + 2 * size], wt[ws, :], preferred_element_type=jnp.float32)
            if drain:
                drain(t, rs)
            return carry

        lax.fori_loop(0, n_mb * tok // TM, tile, 0)

    def out_copy(t, buf, sem):
        m, q = t // (tok // TM), lax.rem(t, tok // TM)
        return pltpu.make_async_copy(buf, y_out.at[m, pl.ds(pl.multiple_of(q * TM, TM), TM)], sem)

    def drain_tile(t, rs):
        for p, buf in enumerate((ln_a, ln_b)):
            @pl.when(lax.rem(t, 2) == p)
            def _():
                @pl.when(t >= 2)
                def _():
                    out_copy(t - 2, buf, osem.at[p]).wait()
                buf[...] = acc[rs, :].astype(jnp.bfloat16)
                out_copy(t, buf, osem.at[p]).start()

    def start(copies):
        for cp in copies:
            cp.start()

    def finish(copies):
        for cp in copies:
            cp.wait()

    def chunk(p, c, u, drain=None):
        size = TN if u is None else LAST[u]
        own = w2_copies(p, size, 0, True, row, 0)
        start(own)

        def wait_h():
            if u is None:
                @pl.when(c < EARLY // 2)
                def _():
                    for m in range(n_mb):
                        for k in range(2):
                            h_early(m, 2 * c + k).wait_recv()

                @pl.when(c >= EARLY // 2)
                def _():
                    for k in range(2):
                        h_pair(2 * c + k).wait_recv()
            else:
                for k in range(2):
                    h_last(k, u).wait_recv()

        w2_sib(p).wait_recv()
        sib_w = w2_copies(p, size, 0, False, sib, 1)
        start(sib_w)
        h0 = h_copies(c, u, 0)
        h1 = h_copies(c, u, 1)
        x_w = w2_copies(p, size, 1, False, xn, 2)
        f_w = w2_copies(p, size, 1, False, xs_row, 3)

        def near_half():
            finish(own)
            finish(sib_w)
            finish(h0)
            product(size, 0)

        @pl.when(diagonal)
        def _():
            start(h0)
            near_half()

        @pl.when(jnp.logical_not(diagonal))
        def _():
            start(h1)

        w2_x(p).wait_recv()
        w2_fwd(p).start()
        if u is None:
            @pl.when(c + WINDOW < n2 - 1)
            def _():
                w2_x(c + WINDOW).start()
                w2_sib(c + WINDOW).start()
        start(x_w)
        wait_h()

        @pl.when(diagonal)
        def _():
            start(h1)

        @pl.when(jnp.logical_not(diagonal))
        def _():
            start(h0)
            near_half()

        w2_fwd(p).wait_recv()
        start(f_w)
        finish(h1)
        finish(x_w)
        finish(f_w)
        product(size, 1, drain)

    def middle(c, carry):
        chunk(c, c, None)

        @pl.when(c == 0)
        def _():
            for p in range(n2 - 1, n2 - 1 + len(LAST)):
                w2_x(p).start()
                w2_sib(p).start()

        return carry

    lax.fori_loop(0, n2 - 1, middle, 0)
    for u in range(len(LAST)):
        chunk(n2 - 1 + u, n2 - 1, u, drain_tile if u == len(LAST) - 1 else None)
    steps = n_mb * tok // TM
    for p, buf in enumerate((ln_a, ln_b)):
        out_copy(steps - 2 + p, buf, osem.at[p]).wait()

    g_move().wait_send()
    for m in range(n_mb):
        x_move(m).wait_send()

    def sent1(s, carry):
        w1_x(s).wait_send()
        w1_sib(s).wait_send()
        w1_fwd(s).wait_send()
        return carry

    def sent2(c, carry):
        w2_x(c).wait_send()
        w2_sib(c).wait_send()
        w2_fwd(c).wait_send()
        return carry

    def sent_early(s, carry):
        for m in range(n_mb):
            h_early(m, s).wait_send()
        return carry

    def sent_pair(s, carry):
        h_pair(s).wait_send()
        return carry

    lax.fori_loop(0, n1, sent1, 0)
    lax.fori_loop(0, n2 - 1, sent2, 0)
    for p in range(n2 - 1, n2 - 1 + len(LAST)):
        sent2(p, 0)
    lax.fori_loop(0, EARLY, sent_early, 0)
    lax.fori_loop(EARLY, n1 - 2, sent_pair, 0)
    for u in range(len(LAST)):
        for k in range(2):
            h_last(k, u).wait_send()


def solution(mesh):
    act_spec = P(None, ("dp", "row"), "col")

    def per_device(x, gamma, w1, w2):
        n_mb, tok, dh = x.shape
        d4, hid = w1.shape
        r4 = w2.shape[0]
        n1, n2 = hid // TN, r4 // TN
        n2p = n2 - 1 + len(LAST)
        nh = (n_mb - 1) * EARLY + n1 - 2 + 2 * len(LAST)
        bf16, f32 = jnp.bfloat16, jnp.float32
        dma = pltpu.SemaphoreType.DMA
        any_spec = pl.BlockSpec(memory_space=pl.ANY)
        shapes = (
            jax.ShapeDtypeStruct((n_mb, tok, dh), bf16),
            jax.ShapeDtypeStruct((n_mb, tok, dh), bf16),
            jax.ShapeDtypeStruct((dh // 128, 128), f32),
            jax.ShapeDtypeStruct((4, n1, d4, TN), bf16),
            jax.ShapeDtypeStruct((4, r4, dh), bf16),
            jax.ShapeDtypeStruct((2, n1, n_mb, TN // SUB, tok, SUB), bf16),
        )
        outs = pl.pallas_call(
            functools.partial(kernel, (n_mb, tok, dh, d4, hid, r4)),
            out_shape=shapes,
            in_specs=[any_spec] * 4,
            out_specs=[any_spec] * len(shapes),
            scratch_shapes=[
                pltpu.VMEM((n_mb * tok, 2 * dh), bf16),
                pltpu.VMEM((8 * d4, TN), bf16),
                pltpu.VMEM((tok, TN), bf16),
                pltpu.VMEM((TM, dh), bf16),
                pltpu.VMEM((TM, dh), bf16),
                pltpu.VMEM((2, dh // 128, 128), f32),
                pltpu.VMEM((2, dh), f32),
                pltpu.VMEM((n_mb * tok, dh), f32),
                dma((n_mb,)), dma((n_mb,)), dma((2,)),
                dma((n1,)), dma((n1,)), dma((n1,)), dma((n1,)), dma((n1,)), dma((n1,)),
                dma((n2p,)), dma((n2p,)), dma((n2p,)), dma((n2p,)), dma((n2p,)), dma((n2p,)),
                dma((nh,)), dma((nh,)),
                dma((8,)), dma((8 * (TN // SUB),)), dma((2,)), dma((4 * (dh // TN),)),
            ],
            compiler_params=pltpu.CompilerParams(collective_id=0, has_side_effects=True, vmem_limit_bytes=67043328),
        )(x, gamma.reshape(dh // 128, 128), w1, w2)
        return outs[0]

    return jax.shard_map(per_device, mesh=mesh, in_specs=(act_spec, P("col"), P("row", "col"), P("row", "col")), out_specs=act_spec, check_vma=False)
```

```python
import functools
import math

import jax
import jax.numpy as jnp
from jax import lax
from jax.experimental import pallas as pl
from jax.experimental.pallas import tpu as pltpu
from jax.sharding import PartitionSpec as P

LN_EPS = 1e-5
MESH = pl.DeviceIdType.MESH
TN = 512
WINDOW = 8
EARLY = 8
TM = 256
SUB = 128
LAST = (256, 128, 128)
TAIL = ((2, 0, 256), (2, 256, 256), (1, 0, 256), (1, 256, 128), (1, 384, 128))
GELU_C = math.sqrt(2 / math.pi)


def kernel(dims, x, g, w1, w2, y_out, xr, gr, w1_all, w2_all, hall,
           z, wt, hout, ln_a, ln_b, g_rows, gv, acc,
           xs, xrs, gs, xs1, xr1, ss1, sr1, fs1, fr1, xs2, xr2, ss2, sr2, fs2, fr2, hs, hr,
           lsem, csem, osem, wsem):
    n_mb, tok, dh, d4, hid, r4 = dims
    d_model = 2 * dh
    n1 = hid // TN
    n2 = r4 // TN
    n_sub = TN // SUB
    last_at = [sum(LAST[:u]) for u in range(len(LAST))]
    full = n2 - TAIL[0][0]
    col = lax.axis_index("col")
    row = lax.axis_index("row")
    far = 1 - col
    sib = row + 1 - 2 * lax.rem(row, 2)
    xn = lax.rem(row + 2, 4)
    xs_row = lax.rem(sib + 2, 4)
    diagonal = row // 2 == col
    to_col, to_x, to_sib = {"col": far}, {"row": xn}, {"row": sib}

    def remote(src, dst, ssem, rsem, dev):
        return pltpu.make_async_remote_copy(src_ref=src, dst_ref=dst, send_sem=ssem, recv_sem=rsem, device_id=dev, device_id_type=MESH)

    def cols(s):
        return pl.ds(pl.multiple_of(lax.rem(s, 2) * r4 + (s // 2) * TN, TN), TN)

    def rows2(p):
        if isinstance(p, int) and p >= full:
            back, at, size = TAIL[p - full]
            return pl.ds((n2 - back) * TN + at, size)
        return pl.ds(pl.multiple_of(p * TN, TN), TN)

    def x_move(m):
        return remote(x.at[m], xr.at[m], xs.at[m], xrs.at[m], to_col)

    def g_move():
        return remote(g, gr, gs.at[0], gs.at[1], to_col)

    def w1_x(s):
        return remote(w1.at[:, cols(s)], w1_all.at[row, s], xs1.at[s], xr1.at[s], to_x)

    def w1_sib(s):
        return remote(w1.at[:, cols(s)], w1_all.at[row, s], ss1.at[s], sr1.at[s], to_sib)

    def w1_fwd(s):
        return remote(w1_all.at[xn, s], w1_all.at[xn, s], fs1.at[s], fr1.at[s], to_sib)

    def w2_x(c):
        return remote(w2.at[rows2(c)], w2_all.at[row, rows2(c)], xs2.at[c], xr2.at[c], to_x)

    def w2_sib(c):
        return remote(w2.at[rows2(c)], w2_all.at[row, rows2(c)], ss2.at[c], sr2.at[c], to_sib)

    def w2_fwd(c):
        return remote(w2_all.at[xn, rows2(c)], w2_all.at[xn, rows2(c)], fs2.at[c], fr2.at[c], to_sib)

    def h_early(m, s):
        q = m * EARLY + s
        return remote(hall.at[col, s, m], hall.at[col, s, m], hs.at[q], hr.at[q], to_col)

    def h_pair(s):
        q = (n_mb - 1) * EARLY + s
        return remote(hall.at[col, s], hall.at[col, s], hs.at[q], hr.at[q], to_col)

    def h_last(k, u):
        s = n1 - 2 + k
        q = (n_mb - 1) * EARLY + n1 - 2 + k * len(LAST) + u
        subs = pl.ds(last_at[u] // SUB, LAST[u] // SUB)
        return remote(hall.at[col, s, :, subs], hall.at[col, s, :, subs], hs.at[q], hr.at[q], to_col)

    barrier = pltpu.get_barrier_semaphore()
    for dev in (to_col, to_x, to_sib):
        pl.semaphore_signal(barrier, inc=1, device_id=dev, device_id_type=MESH)
    pl.semaphore_wait(barrier, 3)

    g_move().start()
    for m in range(n_mb):
        x_move(m).start()

    def first_pieces(s, carry):
        w1_x(s).start()
        w1_sib(s).start()
        return carry

    lax.fori_loop(0, WINDOW, first_pieces, 0)

    def issue_after(s):
        @pl.when(s + WINDOW < n1)
        def _():
            w1_x(s + WINDOW).start()
            w1_sib(s + WINDOW).start()

        @pl.when(s + WINDOW >= n1)
        def _():
            w2_x(s + WINDOW - n1).start()
            w2_sib(s + WINDOW - n1).start()

    def layer_norm(m):
        x_move(m).wait_recv()

        ga = gv[0:1, :]
        gb = gv[1:2, :]

        def tile(t, carry):
            sl = pl.ds(pl.multiple_of(t * TM, TM), TM)
            near = pltpu.make_async_copy(x.at[m, sl], ln_a, lsem.at[0])
            other = pltpu.make_async_copy(xr.at[m, sl], ln_b, lsem.at[1])
            near.start()
            other.start()
            near.wait()
            other.wait()

            def strip(i, carry):
                rs = pl.ds(pl.multiple_of(i * 16, 16), 16)
                a = ln_a[rs, :].astype(jnp.float32)
                b = ln_b[rs, :].astype(jnp.float32)
                mean = (jnp.sum(a, axis=-1, keepdims=True) + jnp.sum(b, axis=-1, keepdims=True)) / d_model
                var = (jnp.sum(a * a, axis=-1, keepdims=True) + jnp.sum(b * b, axis=-1, keepdims=True)) / d_model - mean * mean
                inv = lax.rsqrt(var + LN_EPS)
                zr = pl.ds(pl.multiple_of(m * tok + t * TM + i * 16, 16), 16)
                z[zr, pl.ds(pl.multiple_of(col * dh, 128), dh)] = ((a - mean) * inv * ga).astype(jnp.bfloat16)
                z[zr, pl.ds(pl.multiple_of(far * dh, 128), dh)] = ((b - mean) * inv * gb).astype(jnp.bfloat16)
                return carry

            lax.fori_loop(0, TM // 16, strip, 0)
            return carry

        lax.fori_loop(0, tok // TM, tile, 0)

    def take_piece(s):
        w1_x(s).wait_recv()
        w1_fwd(s).start()
        issue_after(s)
        w1_sib(s).wait_recv()
        w1_fwd(s).wait_recv()

    def wt_copies(s):
        base = lax.rem(s, 2) * (4 * d4)
        sem0 = 4 * lax.rem(s, 2)

        def rows(b):
            return wt.at[pl.ds(pl.multiple_of(base + b * d4, d4), d4)]

        copies = [pltpu.make_async_copy(w1.at[:, cols(s)], rows(row), lsem.at[sem0])]
        for j, b in enumerate((sib, xn, xs_row)):
            copies.append(pltpu.make_async_copy(w1_all.at[b, s], rows(b), lsem.at[sem0 + j + 1]))
        return copies

    def load_wt(s):
        for cp in wt_copies(s):
            cp.start()

    def wait_wt(s):
        for cp in wt_copies(s):
            cp.wait()

    def first_product(m, s):
        base = pl.multiple_of(lax.rem(s, 2) * (4 * d4), 4 * d4)

        def tile(t, carry):
            rs = pl.ds(pl.multiple_of(t * TM, TM), TM)
            zr = pl.ds(pl.multiple_of(m * tok + t * TM, TM), TM)
            u = jnp.dot(z[zr, :], wt[pl.ds(base, 4 * d4), :], preferred_element_type=jnp.float32)
            h = 0.5 * u * (1.0 + jnp.tanh(GELU_C * (u + 0.044715 * (u * u * u))))
            hout[rs, :] = h.astype(jnp.bfloat16)
            return carry

        lax.fori_loop(0, tok // TM, tile, 0)
        copies = [pltpu.make_async_copy(hout.at[:, u * SUB:(u + 1) * SUB], hall.at[col, s, m, u], csem.at[u]) for u in range(n_sub)]
        for cp in copies:
            cp.start()
        for cp in copies:
            cp.wait()

    g_move().wait_recv()
    for i, src in enumerate((g, gr)):
        cp = pltpu.make_async_copy(src, g_rows.at[i], lsem.at[0])
        cp.start()
        cp.wait()
        for j in range(dh // 128):
            gv[i:i + 1, j * 128:(j + 1) * 128] = g_rows[i, j:j + 1, :]
    layer_norm(0)

    def early_a(s, carry):
        take_piece(s)
        load_wt(s)
        wait_wt(s)
        first_product(0, s)
        h_early(0, s).start()
        return carry

    def early_b(s, carry):
        wait_wt(s)

        @pl.when(s + 1 < EARLY)
        def _():
            load_wt(s + 1)

        first_product(1, s)
        h_early(1, s).start()
        return carry

    def both(s):
        take_piece(s)
        load_wt(s)
        wait_wt(s)

        def each(m, carry):
            first_product(m, s)
            return carry

        lax.fori_loop(0, n_mb, each, 0)

    def rest(s, carry):
        both(s)

        @pl.when(s < n1 - 2)
        def _():
            h_pair(s).start()

        return carry

    lax.fori_loop(0, EARLY, early_a, 0)
    layer_norm(1)
    load_wt(0)
    lax.fori_loop(0, EARLY, early_b, 0)
    lax.fori_loop(EARLY, n1, rest, 0)
    for u in range(len(LAST)):
        for k in range(2):
            h_last(k, u).start()

    def init(t, carry):
        m, q = t // (tok // TM), lax.rem(t, tok // TM)
        cp = pltpu.make_async_copy(x.at[m, pl.ds(pl.multiple_of(q * TM, TM), TM)], ln_a, lsem.at[0])
        cp.start()
        cp.wait()
        acc[pl.ds(pl.multiple_of(t * TM, TM), TM), :] = ln_a[...].astype(jnp.float32)
        return carry

    lax.fori_loop(0, n_mb * tok // TM, init, 0)

    def h_copies(c, piece, g):
        at, size = piece
        subs = range(at // SUB, (at + size) // SUB)
        half = row // 2 if g == 0 else 1 - row // 2
        copies = []
        for k in range(2):
            for m in range(n_mb):
                for q, v in enumerate(subs):
                    dst = z.at[pl.ds(m * tok, tok), pl.ds(g * 2 * TN + k * size + q * SUB, SUB)]
                    copies.append(pltpu.make_async_copy(hall.at[half, 2 * c + k, m, v], dst, csem.at[len(copies) + 4 * n_sub * g]))
        return copies

    def w2_copies(p, size, g, src_own, b, lane):
        k = lax.rem(b, 2)
        copies = []
        for i in range(dh // TN):
            rows = pl.ds(pl.multiple_of(g * (dh // TN) * 2 * TN + i * 2 * size + k * size, SUB), size)
            src = (w2.at[rows2(p)] if src_own else w2_all.at[b, rows2(p)]).at[:, i * TN:(i + 1) * TN]
            copies.append(pltpu.make_async_copy(src, wt.at[rows], wsem.at[lane * (dh // TN) + i]))
        return copies

    def product(size, g, drain=None):
        base = g * (dh // TN) * 2 * TN

        def tile(t, carry):
            rs = pl.ds(pl.multiple_of(t * TM, TM), TM)

            for i in range(dh // TN):
                cs = slice(i * TN, (i + 1) * TN)
                ws = slice(base + i * 2 * size, base + (i + 1) * 2 * size)
                acc[rs, cs] += jnp.dot(z[rs, g * 2 * TN:g * 2 * TN + 2 * size], wt[ws, :], preferred_element_type=jnp.float32)
            if drain:
                drain(t, rs)
            return carry

        lax.fori_loop(0, n_mb * tok // TM, tile, 0)

    def out_copy(t, buf, sem):
        m, q = t // (tok // TM), lax.rem(t, tok // TM)
        return pltpu.make_async_copy(buf, y_out.at[m, pl.ds(pl.multiple_of(q * TM, TM), TM)], sem)

    def drain_tile(t, rs):
        for p, buf in enumerate((ln_a, ln_b)):
            @pl.when(lax.rem(t, 2) == p)
            def _():
                @pl.when(t >= 2)
                def _():
                    out_copy(t - 2, buf, osem.at[p]).wait()
                buf[...] = acc[rs, :].astype(jnp.bfloat16)
                out_copy(t, buf, osem.at[p]).start()

    def start(copies):
        for cp in copies:
            cp.start()

    def finish(copies):
        for cp in copies:
            cp.wait()

    def chunk(p, c, piece, drain=None):
        size = piece[1]
        own = w2_copies(p, size, 0, True, row, 0)
        start(own)

        def wait_h():
            if not isinstance(c, int):
                @pl.when(c < EARLY // 2)
                def _():
                    for m in range(n_mb):
                        for k in range(2):
                            h_early(m, 2 * c + k).wait_recv()

                @pl.when(c >= EARLY // 2)
                def _():
                    for k in range(2):
                        h_pair(2 * c + k).wait_recv()
            elif c == n2 - 1:
                for k in range(2):
                    h_last(k, last_at.index(piece[0])).wait_recv()
            elif piece[0] == 0:
                for k in range(2):
                    h_pair(2 * c + k).wait_recv()

        w2_sib(p).wait_recv()
        sib_w = w2_copies(p, size, 0, False, sib, 1)
        start(sib_w)
        h0 = h_copies(c, piece, 0)
        h1 = h_copies(c, piece, 1)
        x_w = w2_copies(p, size, 1, False, xn, 2)
        f_w = w2_copies(p, size, 1, False, xs_row, 3)

        def near_half():
            finish(own)
            finish(sib_w)
            finish(h0)
            product(size, 0)

        @pl.when(diagonal)
        def _():
            start(h0)
            near_half()

        @pl.when(jnp.logical_not(diagonal))
        def _():
            start(h1)

        w2_x(p).wait_recv()
        w2_fwd(p).start()
        start(x_w)
        wait_h()

        @pl.when(diagonal)
        def _():
            start(h1)

        @pl.when(jnp.logical_not(diagonal))
        def _():
            start(h0)
            near_half()

        w2_fwd(p).wait_recv()
        start(f_w)
        finish(h1)
        finish(x_w)
        finish(f_w)
        product(size, 1, drain)

    def middle(c, carry):
        chunk(c, c, (0, TN))

        @pl.when(c == 0)
        def _():
            for p in range(full, full + len(TAIL)):
                w2_x(p).start()
                w2_sib(p).start()

        return carry

    lax.fori_loop(0, full, middle, 0)
    for i, (back, at, size) in enumerate(TAIL):
        chunk(full + i, n2 - back, (at, size), drain_tile if i == len(TAIL) - 1 else None)
    steps = n_mb * tok // TM
    for p, buf in enumerate((ln_a, ln_b)):
        out_copy(steps - 2 + p, buf, osem.at[p]).wait()

    g_move().wait_send()
    for m in range(n_mb):
        x_move(m).wait_send()

    def sent1(s, carry):
        w1_x(s).wait_send()
        w1_sib(s).wait_send()
        w1_fwd(s).wait_send()
        return carry

    def sent2(c, carry):
        w2_x(c).wait_send()
        w2_sib(c).wait_send()
        w2_fwd(c).wait_send()
        return carry

    def sent_early(s, carry):
        for m in range(n_mb):
            h_early(m, s).wait_send()
        return carry

    def sent_pair(s, carry):
        h_pair(s).wait_send()
        return carry

    lax.fori_loop(0, n1, sent1, 0)
    lax.fori_loop(0, full, sent2, 0)
    for p in range(full, full + len(TAIL)):
        sent2(p, 0)
    lax.fori_loop(0, EARLY, sent_early, 0)
    lax.fori_loop(EARLY, n1 - 2, sent_pair, 0)
    for u in range(len(LAST)):
        for k in range(2):
            h_last(k, u).wait_send()


def solution(mesh):
    act_spec = P(None, ("dp", "row"), "col")

    def per_device(x, gamma, w1, w2):
        n_mb, tok, dh = x.shape
        d4, hid = w1.shape
        r4 = w2.shape[0]
        n1, n2 = hid // TN, r4 // TN
        n2p = n2 - TAIL[0][0] + len(TAIL)
        nh = (n_mb - 1) * EARLY + n1 - 2 + 2 * len(LAST)
        bf16, f32 = jnp.bfloat16, jnp.float32
        dma = pltpu.SemaphoreType.DMA
        any_spec = pl.BlockSpec(memory_space=pl.ANY)
        shapes = (
            jax.ShapeDtypeStruct((n_mb, tok, dh), bf16),
            jax.ShapeDtypeStruct((n_mb, tok, dh), bf16),
            jax.ShapeDtypeStruct((dh // 128, 128), f32),
            jax.ShapeDtypeStruct((4, n1, d4, TN), bf16),
            jax.ShapeDtypeStruct((4, r4, dh), bf16),
            jax.ShapeDtypeStruct((2, n1, n_mb, TN // SUB, tok, SUB), bf16),
        )
        outs = pl.pallas_call(
            functools.partial(kernel, (n_mb, tok, dh, d4, hid, r4)),
            out_shape=shapes,
            in_specs=[any_spec] * 4,
            out_specs=[any_spec] * len(shapes),
            scratch_shapes=[
                pltpu.VMEM((n_mb * tok, 2 * dh), bf16),
                pltpu.VMEM((8 * d4, TN), bf16),
                pltpu.VMEM((tok, TN), bf16),
                pltpu.VMEM((TM, dh), bf16),
                pltpu.VMEM((TM, dh), bf16),
                pltpu.VMEM((2, dh // 128, 128), f32),
                pltpu.VMEM((2, dh), f32),
                pltpu.VMEM((n_mb * tok, dh), f32),
                dma((n_mb,)), dma((n_mb,)), dma((2,)),
                dma((n1,)), dma((n1,)), dma((n1,)), dma((n1,)), dma((n1,)), dma((n1,)),
                dma((n2p,)), dma((n2p,)), dma((n2p,)), dma((n2p,)), dma((n2p,)), dma((n2p,)),
                dma((nh,)), dma((nh,)),
                dma((8,)), dma((8 * (TN // SUB),)), dma((2,)), dma((4 * (dh // TN),)),
            ],
            compiler_params=pltpu.CompilerParams(collective_id=0, has_side_effects=True, vmem_limit_bytes=67043328),
        )(x, gamma.reshape(dh // 128, 128), w1, w2)
        return outs[0]

    return jax.shard_map(per_device, mesh=mesh, in_specs=(act_spec, P("col"), P("row", "col"), P("row", "col")), out_specs=act_spec, check_vma=False)
```

```python
import functools
import math

import jax
import jax.numpy as jnp
from jax import lax
from jax.experimental import pallas as pl
from jax.experimental.pallas import tpu as pltpu
from jax.sharding import PartitionSpec as P

LN_EPS = 1e-5
MESH = pl.DeviceIdType.MESH
TN = 512
WINDOW = 8
EARLY = 8
TM = 256
SUB = 128
LAST = (256, 128, 128)
TAIL = ((2, 0, 256), (2, 256, 256), (1, 0, 256), (1, 256, 128), (1, 384, 128))
GELU_C = math.sqrt(2 / math.pi)


def kernel(dims, x, g, w1, w2, y_out, xr, gr, w1_all, w2_all, hall,
           z, wt, hout, ln_a, ln_b, g_rows, gv, acc,
           xs, xrs, gs, xs1, xr1, ss1, sr1, fs1, fr1, xs2, xr2, ss2, sr2, fs2, fr2, hs, hr,
           lsem, csem, osem, wsem):
    n_mb, tok, dh, d4, hid, r4 = dims
    d_model = 2 * dh
    n1 = hid // TN
    n2 = r4 // TN
    n_sub = TN // SUB
    last_at = [sum(LAST[:u]) for u in range(len(LAST))]
    full = n2 - TAIL[0][0]
    col = lax.axis_index("col")
    row = lax.axis_index("row")
    far = 1 - col
    sib = row + 1 - 2 * lax.rem(row, 2)
    xn = lax.rem(row + 2, 4)
    xs_row = lax.rem(sib + 2, 4)
    diagonal = row // 2 == col
    to_col, to_x, to_sib = {"col": far}, {"row": xn}, {"row": sib}

    def remote(src, dst, ssem, rsem, dev):
        return pltpu.make_async_remote_copy(src_ref=src, dst_ref=dst, send_sem=ssem, recv_sem=rsem, device_id=dev, device_id_type=MESH)

    def cols(s):
        return pl.ds(pl.multiple_of(lax.rem(s, 2) * r4 + (s // 2) * TN, TN), TN)

    def rows2(p):
        if isinstance(p, int) and p >= full:
            back, at, size = TAIL[p - full]
            return pl.ds((n2 - back) * TN + at, size)
        return pl.ds(pl.multiple_of(p * TN, TN), TN)

    def x_move(m):
        return remote(x.at[m], xr.at[m], xs.at[m], xrs.at[m], to_col)

    def g_move():
        return remote(g, gr, gs.at[0], gs.at[1], to_col)

    def w1_x(s):
        return remote(w1.at[:, cols(s)], w1_all.at[row, s], xs1.at[s], xr1.at[s], to_x)

    def w1_sib(s):
        return remote(w1.at[:, cols(s)], w1_all.at[row, s], ss1.at[s], sr1.at[s], to_sib)

    def w1_fwd(s):
        return remote(w1_all.at[xn, s], w1_all.at[xn, s], fs1.at[s], fr1.at[s], to_sib)

    def w2_x(c):
        return remote(w2.at[rows2(c)], w2_all.at[row, rows2(c)], xs2.at[c], xr2.at[c], to_x)

    def w2_sib(c):
        return remote(w2.at[rows2(c)], w2_all.at[row, rows2(c)], ss2.at[c], sr2.at[c], to_sib)

    def w2_fwd(c):
        return remote(w2_all.at[xn, rows2(c)], w2_all.at[xn, rows2(c)], fs2.at[c], fr2.at[c], to_sib)

    def h_early(m, s):
        q = m * EARLY + s
        return remote(hall.at[col, s, m], hall.at[col, s, m], hs.at[q], hr.at[q], to_col)

    def h_pair(s):
        q = (n_mb - 1) * EARLY + s
        return remote(hall.at[col, s], hall.at[col, s], hs.at[q], hr.at[q], to_col)

    def h_last(k, u):
        s = n1 - 2 + k
        q = (n_mb - 1) * EARLY + n1 - 2 + k * len(LAST) + u
        subs = pl.ds(last_at[u] // SUB, LAST[u] // SUB)
        return remote(hall.at[col, s, :, subs], hall.at[col, s, :, subs], hs.at[q], hr.at[q], to_col)

    def h_end(k, m):
        q = (n_mb - 1) * EARLY + n1 - 2 + 2 * len(LAST) + k * n_mb + m
        u = len(LAST) - 1
        ref = hall.at[col, n1 - 2 + k, m, pl.ds(last_at[u] // SUB, LAST[u] // SUB)]
        return remote(ref, ref, hs.at[q], hr.at[q], to_col)

    p_end = full + len(TAIL) - 1
    split = (dh // TN + 1) // 2
    end_parts = (range(split), range(split, dh // TN))

    def end_ref(ref, part):
        i = end_parts[part]
        return ref.at[rows2(p_end), i[0] * TN:(i[-1] + 1) * TN]

    def w2_x_end(part):
        return remote(end_ref(w2, part), end_ref(w2_all.at[row], part), xs2.at[p_end + part], xr2.at[p_end + part], to_x)

    def w2_fwd_end(part):
        return remote(end_ref(w2_all.at[xn], part), end_ref(w2_all.at[xn], part), fs2.at[p_end + part], fr2.at[p_end + part], to_sib)

    barrier = pltpu.get_barrier_semaphore()
    for dev in (to_col, to_x, to_sib):
        pl.semaphore_signal(barrier, inc=1, device_id=dev, device_id_type=MESH)
    pl.semaphore_wait(barrier, 3)

    g_move().start()
    for m in range(n_mb):
        x_move(m).start()

    def first_pieces(s, carry):
        w1_x(s).start()
        w1_sib(s).start()
        return carry

    lax.fori_loop(0, WINDOW, first_pieces, 0)

    def issue_after(s):
        @pl.when(s + WINDOW < n1)
        def _():
            w1_x(s + WINDOW).start()
            w1_sib(s + WINDOW).start()

        @pl.when(s + WINDOW >= n1)
        def _():
            w2_x(s + WINDOW - n1).start()
            w2_sib(s + WINDOW - n1).start()

    def layer_norm(m):
        x_move(m).wait_recv()

        ga = gv[0:1, :]
        gb = gv[1:2, :]

        def tile(t, carry):
            sl = pl.ds(pl.multiple_of(t * TM, TM), TM)
            near = pltpu.make_async_copy(x.at[m, sl], ln_a, lsem.at[0])
            other = pltpu.make_async_copy(xr.at[m, sl], ln_b, lsem.at[1])
            near.start()
            other.start()
            near.wait()
            other.wait()

            def strip(i, carry):
                rs = pl.ds(pl.multiple_of(i * 16, 16), 16)
                a = ln_a[rs, :].astype(jnp.float32)
                b = ln_b[rs, :].astype(jnp.float32)
                mean = (jnp.sum(a, axis=-1, keepdims=True) + jnp.sum(b, axis=-1, keepdims=True)) / d_model
                var = (jnp.sum(a * a, axis=-1, keepdims=True) + jnp.sum(b * b, axis=-1, keepdims=True)) / d_model - mean * mean
                inv = lax.rsqrt(var + LN_EPS)
                zr = pl.ds(pl.multiple_of(m * tok + t * TM + i * 16, 16), 16)
                z[zr, pl.ds(pl.multiple_of(col * dh, 128), dh)] = ((a - mean) * inv * ga).astype(jnp.bfloat16)
                z[zr, pl.ds(pl.multiple_of(far * dh, 128), dh)] = ((b - mean) * inv * gb).astype(jnp.bfloat16)
                return carry

            lax.fori_loop(0, TM // 16, strip, 0)
            return carry

        lax.fori_loop(0, tok // TM, tile, 0)

    def take_piece(s):
        w1_x(s).wait_recv()
        w1_fwd(s).start()
        issue_after(s)
        w1_sib(s).wait_recv()
        w1_fwd(s).wait_recv()

    def wt_copies(s):
        base = lax.rem(s, 2) * (4 * d4)
        sem0 = 4 * lax.rem(s, 2)

        def rows(b):
            return wt.at[pl.ds(pl.multiple_of(base + b * d4, d4), d4)]

        copies = [pltpu.make_async_copy(w1.at[:, cols(s)], rows(row), lsem.at[sem0])]
        for j, b in enumerate((sib, xn, xs_row)):
            copies.append(pltpu.make_async_copy(w1_all.at[b, s], rows(b), lsem.at[sem0 + j + 1]))
        return copies

    def load_wt(s):
        for cp in wt_copies(s):
            cp.start()

    def wait_wt(s):
        for cp in wt_copies(s):
            cp.wait()

    def first_product(m, s):
        base = pl.multiple_of(lax.rem(s, 2) * (4 * d4), 4 * d4)

        def tile(t, carry):
            rs = pl.ds(pl.multiple_of(t * TM, TM), TM)
            zr = pl.ds(pl.multiple_of(m * tok + t * TM, TM), TM)
            u = jnp.dot(z[zr, :], wt[pl.ds(base, 4 * d4), :], preferred_element_type=jnp.float32)
            h = 0.5 * u * (1.0 + jnp.tanh(GELU_C * (u + 0.044715 * (u * u * u))))
            hout[rs, :] = h.astype(jnp.bfloat16)
            return carry

        lax.fori_loop(0, tok // TM, tile, 0)
        copies = [pltpu.make_async_copy(hout.at[:, u * SUB:(u + 1) * SUB], hall.at[col, s, m, u], csem.at[u]) for u in range(n_sub)]
        for cp in copies:
            cp.start()
        for cp in copies:
            cp.wait()

    g_move().wait_recv()
    for i, src in enumerate((g, gr)):
        cp = pltpu.make_async_copy(src, g_rows.at[i], lsem.at[0])
        cp.start()
        cp.wait()
        for j in range(dh // 128):
            gv[i:i + 1, j * 128:(j + 1) * 128] = g_rows[i, j:j + 1, :]
    layer_norm(0)

    def early_a(s, carry):
        take_piece(s)
        load_wt(s)
        wait_wt(s)
        first_product(0, s)
        h_early(0, s).start()
        return carry

    def early_b(s, carry):
        wait_wt(s)

        @pl.when(s + 1 < EARLY)
        def _():
            load_wt(s + 1)

        first_product(1, s)
        h_early(1, s).start()
        return carry

    def both(s):
        take_piece(s)
        load_wt(s)
        wait_wt(s)

        def each(m, carry):
            first_product(m, s)
            return carry

        lax.fori_loop(0, n_mb, each, 0)

    def rest(s, carry):
        both(s)

        @pl.when(s < n1 - 2)
        def _():
            h_pair(s).start()

        return carry

    lax.fori_loop(0, EARLY, early_a, 0)
    layer_norm(1)
    load_wt(0)
    lax.fori_loop(0, EARLY, early_b, 0)
    lax.fori_loop(EARLY, n1, rest, 0)
    for u in range(len(LAST) - 1):
        for k in range(2):
            h_last(k, u).start()
    for m in range(n_mb):
        for k in range(2):
            h_end(k, m).start()

    def init(t, carry):
        m, q = t // (tok // TM), lax.rem(t, tok // TM)
        cp = pltpu.make_async_copy(x.at[m, pl.ds(pl.multiple_of(q * TM, TM), TM)], ln_a, lsem.at[0])
        cp.start()
        cp.wait()
        acc[pl.ds(pl.multiple_of(t * TM, TM), TM), :] = ln_a[...].astype(jnp.float32)
        return carry

    lax.fori_loop(0, n_mb * tok // TM, init, 0)

    def h_copies(c, piece, g, mbs=None):
        at, size = piece
        subs = range(at // SUB, (at + size) // SUB)
        half = row // 2 if g == 0 else 1 - row // 2
        copies = []
        for k in range(2):
            for m in mbs or range(n_mb):
                for q, v in enumerate(subs):
                    dst = z.at[pl.ds(m * tok, tok), pl.ds(g * 2 * TN + k * size + q * SUB, SUB)]
                    copies.append(pltpu.make_async_copy(hall.at[half, 2 * c + k, m, v], dst, csem.at[((g * 2 + k) * n_mb + m) * n_sub + q]))
        return copies

    def w2_copies(p, size, g, src_own, b, lane, parts=None):
        k = lax.rem(b, 2)
        copies = []
        for i in parts or range(dh // TN):
            rows = pl.ds(pl.multiple_of(g * (dh // TN) * 2 * TN + i * 2 * size + k * size, SUB), size)
            src = (w2.at[rows2(p)] if src_own else w2_all.at[b, rows2(p)]).at[:, i * TN:(i + 1) * TN]
            copies.append(pltpu.make_async_copy(src, wt.at[rows], wsem.at[lane * (dh // TN) + i]))
        return copies

    def product(size, g, drain=None, mbs=None, parts=None):
        base = g * (dh // TN) * 2 * TN

        def tile(t, carry):
            rs = pl.ds(pl.multiple_of(t * TM, TM), TM)

            for i in parts or range(dh // TN):
                cs = slice(i * TN, (i + 1) * TN)
                ws = slice(base + i * 2 * size, base + (i + 1) * 2 * size)
                acc[rs, cs] += jnp.dot(z[rs, g * 2 * TN:g * 2 * TN + 2 * size], wt[ws, :], preferred_element_type=jnp.float32)
            if drain:
                drain(t, rs)
            return carry

        mbs = mbs or range(n_mb)
        lax.fori_loop(mbs[0] * tok // TM, (mbs[-1] + 1) * tok // TM, tile, 0)

    def out_copy(t, buf, sem):
        m, q = t // (tok // TM), lax.rem(t, tok // TM)
        return pltpu.make_async_copy(buf, y_out.at[m, pl.ds(pl.multiple_of(q * TM, TM), TM)], sem)

    def drain_tile(t, rs):
        for p, buf in enumerate((ln_a, ln_b)):
            @pl.when(lax.rem(t, 2) == p)
            def _():
                @pl.when(t >= 2)
                def _():
                    out_copy(t - 2, buf, osem.at[p]).wait()
                buf[...] = acc[rs, :].astype(jnp.bfloat16)
                out_copy(t, buf, osem.at[p]).start()

    def start(copies):
        for cp in copies:
            cp.start()

    def finish(copies):
        for cp in copies:
            cp.wait()

    def chunk(p, c, piece, drain=None):
        size = piece[1]
        own = w2_copies(p, size, 0, True, row, 0)
        start(own)

        def wait_h():
            if not isinstance(c, int):
                @pl.when(c < EARLY // 2)
                def _():
                    for m in range(n_mb):
                        for k in range(2):
                            h_early(m, 2 * c + k).wait_recv()

                @pl.when(c >= EARLY // 2)
                def _():
                    for k in range(2):
                        h_pair(2 * c + k).wait_recv()
            elif c == n2 - 1:
                for k in range(2):
                    h_last(k, last_at.index(piece[0])).wait_recv()
            elif piece[0] == 0:
                for k in range(2):
                    h_pair(2 * c + k).wait_recv()

        w2_sib(p).wait_recv()
        sib_w = w2_copies(p, size, 0, False, sib, 1)
        start(sib_w)
        h0 = h_copies(c, piece, 0)
        h1 = h_copies(c, piece, 1)
        x_w = w2_copies(p, size, 1, False, xn, 2)
        f_w = w2_copies(p, size, 1, False, xs_row, 3)

        def near_half():
            finish(own)
            finish(sib_w)
            finish(h0)
            product(size, 0)

        @pl.when(diagonal)
        def _():
            start(h0)
            near_half()

        @pl.when(jnp.logical_not(diagonal))
        def _():
            start(h1)

        w2_x(p).wait_recv()
        w2_fwd(p).start()
        start(x_w)
        wait_h()

        @pl.when(diagonal)
        def _():
            start(h1)

        @pl.when(jnp.logical_not(diagonal))
        def _():
            start(h0)
            near_half()

        w2_fwd(p).wait_recv()
        start(f_w)
        finish(h1)
        finish(x_w)
        finish(f_w)
        product(size, 1, drain)

    def middle(c, carry):
        chunk(c, c, (0, TN))

        @pl.when(c == 0)
        def _():
            for p in range(full, p_end):
                w2_x(p).start()
                w2_sib(p).start()
            for part in range(2):
                w2_x_end(part).start()
            w2_sib(p_end).start()

        return carry

    lax.fori_loop(0, full, middle, 0)
    for i, (back, at, size) in enumerate(TAIL[:-1]):
        chunk(full + i, n2 - back, (at, size))

    def end_chunk():
        c, piece, size = n2 - 1, TAIL[-1][1:], TAIL[-1][2]
        own = w2_copies(p_end, size, 0, True, row, 0)
        start(own)
        w2_sib(p_end).wait_recv()
        sib_w = w2_copies(p_end, size, 0, False, sib, 1)
        start(sib_w)
        h0 = [h_copies(c, piece, 0, (m,)) for m in range(n_mb)]
        h1 = [h_copies(c, piece, 1, (m,)) for m in range(n_mb)]
        x_w = [w2_copies(p_end, size, 1, False, xn, 2, i) for i in end_parts]
        f_w = [w2_copies(p_end, size, 1, False, xs_row, 3, i) for i in end_parts]

        def wait_h(m):
            for k in range(2):
                h_end(k, m).wait_recv()

        @pl.when(diagonal)
        def _():
            for m in range(n_mb):
                start(h0[m])
            finish(own)
            finish(sib_w)
            for m in range(n_mb):
                finish(h0[m])
            product(size, 0)

        @pl.when(jnp.logical_not(diagonal))
        def _():
            for m in range(n_mb):
                start(h1[m])
            finish(own)
            finish(sib_w)

        wait_h(0)

        @pl.when(diagonal)
        def _():
            start(h1[0])

        @pl.when(jnp.logical_not(diagonal))
        def _():
            start(h0[0])
            finish(h0[0])
            product(size, 0, None, (0,))

        w2_x_end(0).wait_recv()
        w2_fwd_end(0).start()
        start(x_w[0])
        w2_fwd_end(0).wait_recv()
        start(f_w[0])
        finish(h1[0])
        finish(x_w[0])
        finish(f_w[0])
        product(size, 1, None, (0,), end_parts[0])

        @pl.when(jnp.logical_not(diagonal))
        def _():
            finish(h1[1])
            product(size, 1, None, (1,), end_parts[0])

        w2_x_end(1).wait_recv()
        w2_fwd_end(1).start()
        start(x_w[1])
        wait_h(1)

        @pl.when(diagonal)
        def _():
            start(h1[1])
            finish(h1[1])
            product(size, 1, None, (1,), end_parts[0])

        @pl.when(jnp.logical_not(diagonal))
        def _():
            start(h0[1])
            finish(h0[1])
            product(size, 0, None, (1,))

        w2_fwd_end(1).wait_recv()
        start(f_w[1])
        finish(x_w[1])
        finish(f_w[1])
        product(size, 1, drain_tile, None, end_parts[1])

    end_chunk()
    steps = n_mb * tok // TM
    for p, buf in enumerate((ln_a, ln_b)):
        out_copy(steps - 2 + p, buf, osem.at[p]).wait()

    g_move().wait_send()
    for m in range(n_mb):
        x_move(m).wait_send()

    def sent1(s, carry):
        w1_x(s).wait_send()
        w1_sib(s).wait_send()
        w1_fwd(s).wait_send()
        return carry

    def sent2(c, carry):
        w2_x(c).wait_send()
        w2_sib(c).wait_send()
        w2_fwd(c).wait_send()
        return carry

    def sent_early(s, carry):
        for m in range(n_mb):
            h_early(m, s).wait_send()
        return carry

    def sent_pair(s, carry):
        h_pair(s).wait_send()
        return carry

    lax.fori_loop(0, n1, sent1, 0)
    lax.fori_loop(0, full, sent2, 0)
    for p in range(full, p_end):
        sent2(p, 0)
    for part in range(2):
        w2_x_end(part).wait_send()
        w2_fwd_end(part).wait_send()
    w2_sib(p_end).wait_send()
    lax.fori_loop(0, EARLY, sent_early, 0)
    lax.fori_loop(EARLY, n1 - 2, sent_pair, 0)
    for k in range(2):
        for u in range(len(LAST) - 1):
            h_last(k, u).wait_send()
        for m in range(n_mb):
            h_end(k, m).wait_send()


def solution(mesh):
    act_spec = P(None, ("dp", "row"), "col")

    def per_device(x, gamma, w1, w2):
        n_mb, tok, dh = x.shape
        d4, hid = w1.shape
        r4 = w2.shape[0]
        n1, n2 = hid // TN, r4 // TN
        n2p = n2 - TAIL[0][0] + len(TAIL) + 1
        nh = (n_mb - 1) * EARLY + n1 - 2 + 2 * len(LAST) + 2 * n_mb
        bf16, f32 = jnp.bfloat16, jnp.float32
        dma = pltpu.SemaphoreType.DMA
        any_spec = pl.BlockSpec(memory_space=pl.ANY)
        shapes = (
            jax.ShapeDtypeStruct((n_mb, tok, dh), bf16),
            jax.ShapeDtypeStruct((n_mb, tok, dh), bf16),
            jax.ShapeDtypeStruct((dh // 128, 128), f32),
            jax.ShapeDtypeStruct((4, n1, d4, TN), bf16),
            jax.ShapeDtypeStruct((4, r4, dh), bf16),
            jax.ShapeDtypeStruct((2, n1, n_mb, TN // SUB, tok, SUB), bf16),
        )
        outs = pl.pallas_call(
            functools.partial(kernel, (n_mb, tok, dh, d4, hid, r4)),
            out_shape=shapes,
            in_specs=[any_spec] * 4,
            out_specs=[any_spec] * len(shapes),
            scratch_shapes=[
                pltpu.VMEM((n_mb * tok, 2 * dh), bf16),
                pltpu.VMEM((8 * d4, TN), bf16),
                pltpu.VMEM((tok, TN), bf16),
                pltpu.VMEM((TM, dh), bf16),
                pltpu.VMEM((TM, dh), bf16),
                pltpu.VMEM((2, dh // 128, 128), f32),
                pltpu.VMEM((2, dh), f32),
                pltpu.VMEM((n_mb * tok, dh), f32),
                dma((n_mb,)), dma((n_mb,)), dma((2,)),
                dma((n1,)), dma((n1,)), dma((n1,)), dma((n1,)), dma((n1,)), dma((n1,)),
                dma((n2p,)), dma((n2p,)), dma((n2p,)), dma((n2p,)), dma((n2p,)), dma((n2p,)),
                dma((nh,)), dma((nh,)),
                dma((8,)), dma((8 * (TN // SUB),)), dma((2,)), dma((4 * (dh // TN),)),
            ],
            compiler_params=pltpu.CompilerParams(collective_id=0, has_side_effects=True, vmem_limit_bytes=67043328),
        )(x, gamma.reshape(dh // 128, 128), w1, w2)
        return outs[0]

    return jax.shard_map(per_device, mesh=mesh, in_specs=(act_spec, P("col"), P("row", "col"), P("row", "col")), out_specs=act_spec, check_vma=False)
```

```python
import functools
import math

import jax
import jax.numpy as jnp
from jax import lax
from jax.experimental import pallas as pl
from jax.experimental.pallas import tpu as pltpu
from jax.sharding import PartitionSpec as P

LN_EPS = 1e-5
MESH = pl.DeviceIdType.MESH
TN = 512
TW = 2 * TN
WINDOW = 4
EARLY = 8
TM = 256
SUB = 128
LAST = (256, 128, 128)
TAIL = ((2, 0, 256), (2, 256, 256), (1, 0, 256), (1, 256, 128), (1, 384, 128))
GELU_C = math.sqrt(2 / math.pi)


def kernel(dims, x, g, w1, w2, y_out, xr, gr, w1_all, w2_all, hall,
           z, wt, hout, ln_a, ln_b, g_rows, gv, acc,
           xs, xrs, gs, xs1, xr1, ss1, sr1, fs1, fr1, xs2, xr2, ss2, sr2, fs2, fr2, hs, hr,
           lsem, csem, osem, wsem):
    n_mb, tok, dh, d4, hid, r4 = dims
    d_model = 2 * dh
    n1 = hid // TN
    n2 = r4 // TN
    nq = hid // TW
    n_sub = TN // SUB
    last_at = [sum(LAST[:u]) for u in range(len(LAST))]
    full = n2 - TAIL[0][0]
    col = lax.axis_index("col")
    row = lax.axis_index("row")
    far = 1 - col
    sib = row + 1 - 2 * lax.rem(row, 2)
    xn = lax.rem(row + 2, 4)
    xs_row = lax.rem(sib + 2, 4)
    diagonal = row // 2 == col
    to_col, to_x, to_sib = {"col": far}, {"row": xn}, {"row": sib}

    def remote(src, dst, ssem, rsem, dev):
        return pltpu.make_async_remote_copy(src_ref=src, dst_ref=dst, send_sem=ssem, recv_sem=rsem, device_id=dev, device_id_type=MESH)

    def cols(s):
        return pl.ds(pl.multiple_of(lax.rem(s, 2) * r4 + (s // 2) * TN, TN), TN)

    def rows2(p):
        if isinstance(p, int) and p >= full:
            back, at, size = TAIL[p - full]
            return pl.ds((n2 - back) * TN + at, size)
        return pl.ds(pl.multiple_of(p * TN, TN), TN)

    def x_move(m):
        return remote(x.at[m], xr.at[m], xs.at[m], xrs.at[m], to_col)

    def g_move():
        return remote(g, gr, gs.at[0], gs.at[1], to_col)

    def cols_in(q):
        return pl.ds(pl.multiple_of(lax.rem(q, 2) * r4 + (q // 2) * TW, TW), TW)

    def step_of(t):
        q = t // 2
        return 2 * (2 * (q // 2) + lax.rem(t, 2)) + lax.rem(q, 2)

    def w1_x(q):
        return remote(w1.at[:, cols_in(q)], w1_all.at[row, q], xs1.at[q], xr1.at[q], to_x)

    def w1_sib(q):
        return remote(w1.at[:, cols_in(q)], w1_all.at[row, q], ss1.at[q], sr1.at[q], to_sib)

    def w1_fwd(q):
        return remote(w1_all.at[xn, q], w1_all.at[xn, q], fs1.at[q], fr1.at[q], to_sib)

    def w2_x(c):
        return remote(w2.at[rows2(c)], w2_all.at[row, rows2(c)], xs2.at[c], xr2.at[c], to_x)

    def w2_sib(c):
        return remote(w2.at[rows2(c)], w2_all.at[row, rows2(c)], ss2.at[c], sr2.at[c], to_sib)

    def w2_fwd(c):
        return remote(w2_all.at[xn, rows2(c)], w2_all.at[xn, rows2(c)], fs2.at[c], fr2.at[c], to_sib)

    def h_early(m, s):
        q = m * EARLY + s
        return remote(hall.at[col, s, m], hall.at[col, s, m], hs.at[q], hr.at[q], to_col)

    def h_pair(s):
        q = (n_mb - 1) * EARLY + s
        return remote(hall.at[col, s], hall.at[col, s], hs.at[q], hr.at[q], to_col)

    def h_last(k, u):
        s = n1 - 2 + k
        q = (n_mb - 1) * EARLY + n1 - 2 + k * len(LAST) + u
        subs = pl.ds(last_at[u] // SUB, LAST[u] // SUB)
        return remote(hall.at[col, s, :, subs], hall.at[col, s, :, subs], hs.at[q], hr.at[q], to_col)

    barrier = pltpu.get_barrier_semaphore()
    for dev in (to_col, to_x, to_sib):
        pl.semaphore_signal(barrier, inc=1, device_id=dev, device_id_type=MESH)
    pl.semaphore_wait(barrier, 3)

    g_move().start()
    for m in range(n_mb):
        x_move(m).start()

    def first_pieces(s, carry):
        w1_x(s).start()
        w1_sib(s).start()
        return carry

    lax.fori_loop(0, WINDOW, first_pieces, 0)

    def issue_after(q):
        @pl.when(q + WINDOW < nq)
        def _():
            w1_x(q + WINDOW).start()
            w1_sib(q + WINDOW).start()

        @pl.when(q + WINDOW >= nq)
        def _():
            for i in range(2):
                w2_x(2 * (q + WINDOW - nq) + i).start()
                w2_sib(2 * (q + WINDOW - nq) + i).start()

    def layer_norm(m):
        x_move(m).wait_recv()

        ga = gv[0:1, :]
        gb = gv[1:2, :]

        def tile(t, carry):
            sl = pl.ds(pl.multiple_of(t * TM, TM), TM)
            near = pltpu.make_async_copy(x.at[m, sl], ln_a, lsem.at[0])
            other = pltpu.make_async_copy(xr.at[m, sl], ln_b, lsem.at[1])
            near.start()
            other.start()
            near.wait()
            other.wait()

            def strip(i, carry):
                rs = pl.ds(pl.multiple_of(i * 16, 16), 16)
                a = ln_a[rs, :].astype(jnp.float32)
                b = ln_b[rs, :].astype(jnp.float32)
                mean = (jnp.sum(a, axis=-1, keepdims=True) + jnp.sum(b, axis=-1, keepdims=True)) / d_model
                var = (jnp.sum(a * a, axis=-1, keepdims=True) + jnp.sum(b * b, axis=-1, keepdims=True)) / d_model - mean * mean
                inv = lax.rsqrt(var + LN_EPS)
                zr = pl.ds(pl.multiple_of(m * tok + t * TM + i * 16, 16), 16)
                z[zr, pl.ds(pl.multiple_of(col * dh, 128), dh)] = ((a - mean) * inv * ga).astype(jnp.bfloat16)
                z[zr, pl.ds(pl.multiple_of(far * dh, 128), dh)] = ((b - mean) * inv * gb).astype(jnp.bfloat16)
                return carry

            lax.fori_loop(0, TM // 16, strip, 0)
            return carry

        lax.fori_loop(0, tok // TM, tile, 0)

    def take_piece(s):
        w1_x(s).wait_recv()
        w1_fwd(s).start()
        issue_after(s)
        w1_sib(s).wait_recv()
        w1_fwd(s).wait_recv()

    def wt_copies(t):
        base = lax.rem(t, 2) * (4 * d4)
        sem0 = 4 * lax.rem(t, 2)
        half = pl.ds(pl.multiple_of(lax.rem(t, 2) * TN, TN), TN)

        def rows(b):
            return wt.at[pl.ds(pl.multiple_of(base + b * d4, d4), d4)]

        copies = [pltpu.make_async_copy(w1.at[:, cols(step_of(t))], rows(row), lsem.at[sem0])]
        for j, b in enumerate((sib, xn, xs_row)):
            copies.append(pltpu.make_async_copy(w1_all.at[b, t // 2, :, half], rows(b), lsem.at[sem0 + j + 1]))
        return copies

    def load_wt(s):
        for cp in wt_copies(s):
            cp.start()

    def wait_wt(s):
        for cp in wt_copies(s):
            cp.wait()

    def first_product(m, t):
        s = step_of(t)
        base = pl.multiple_of(lax.rem(t, 2) * (4 * d4), 4 * d4)

        def tile(i, carry):
            rs = pl.ds(pl.multiple_of(i * TM, TM), TM)
            zr = pl.ds(pl.multiple_of(m * tok + i * TM, TM), TM)
            u = jnp.dot(z[zr, :], wt[pl.ds(base, 4 * d4), :], preferred_element_type=jnp.float32)
            h = 0.5 * u * (1.0 + jnp.tanh(GELU_C * (u + 0.044715 * (u * u * u))))
            hout[rs, :] = h.astype(jnp.bfloat16)
            return carry

        lax.fori_loop(0, tok // TM, tile, 0)
        copies = [pltpu.make_async_copy(hout.at[:, u * SUB:(u + 1) * SUB], hall.at[col, s, m, u], csem.at[u]) for u in range(n_sub)]
        for cp in copies:
            cp.start()
        for cp in copies:
            cp.wait()

    g_move().wait_recv()
    for i, src in enumerate((g, gr)):
        cp = pltpu.make_async_copy(src, g_rows.at[i], lsem.at[0])
        cp.start()
        cp.wait()
        for j in range(dh // 128):
            gv[i:i + 1, j * 128:(j + 1) * 128] = g_rows[i, j:j + 1, :]
    layer_norm(0)

    def take_at(t):
        @pl.when(lax.rem(t, 2) == 0)
        def _():
            take_piece(t // 2)

    def early_a(t, carry):
        take_at(t)
        load_wt(t)
        wait_wt(t)
        first_product(0, t)
        h_early(0, step_of(t)).start()
        return carry

    def early_b(t, carry):
        wait_wt(t)

        @pl.when(t + 1 < EARLY)
        def _():
            load_wt(t + 1)

        first_product(1, t)
        h_early(1, step_of(t)).start()
        return carry

    def rest(t, carry):
        take_at(t)
        load_wt(t)
        wait_wt(t)

        def each(m, carry):
            first_product(m, t)
            return carry

        lax.fori_loop(0, n_mb, each, 0)

        @pl.when(step_of(t) < n1 - 2)
        def _():
            h_pair(step_of(t)).start()

        return carry

    lax.fori_loop(0, EARLY, early_a, 0)
    layer_norm(1)
    load_wt(0)
    lax.fori_loop(0, EARLY, early_b, 0)
    lax.fori_loop(EARLY, n1, rest, 0)
    for u in range(len(LAST)):
        for k in range(2):
            h_last(k, u).start()

    def init(t, carry):
        m, q = t // (tok // TM), lax.rem(t, tok // TM)
        cp = pltpu.make_async_copy(x.at[m, pl.ds(pl.multiple_of(q * TM, TM), TM)], ln_a, lsem.at[0])
        cp.start()
        cp.wait()
        acc[pl.ds(pl.multiple_of(t * TM, TM), TM), :] = ln_a[...].astype(jnp.float32)
        return carry

    lax.fori_loop(0, n_mb * tok // TM, init, 0)

    def h_copies(c, piece, g):
        at, size = piece
        subs = range(at // SUB, (at + size) // SUB)
        half = row // 2 if g == 0 else 1 - row // 2
        copies = []
        for k in range(2):
            for m in range(n_mb):
                for q, v in enumerate(subs):
                    dst = z.at[pl.ds(m * tok, tok), pl.ds(g * 2 * TN + k * size + q * SUB, SUB)]
                    copies.append(pltpu.make_async_copy(hall.at[half, 2 * c + k, m, v], dst, csem.at[len(copies) + 4 * n_sub * g]))
        return copies

    def w2_copies(p, size, g, src_own, b, lane):
        k = lax.rem(b, 2)
        copies = []
        for i in range(dh // TN):
            rows = pl.ds(pl.multiple_of(g * (dh // TN) * 2 * TN + i * 2 * size + k * size, SUB), size)
            src = (w2.at[rows2(p)] if src_own else w2_all.at[b, rows2(p)]).at[:, i * TN:(i + 1) * TN]
            copies.append(pltpu.make_async_copy(src, wt.at[rows], wsem.at[lane * (dh // TN) + i]))
        return copies

    def product(size, g, drain=None):
        base = g * (dh // TN) * 2 * TN

        def tile(t, carry):
            rs = pl.ds(pl.multiple_of(t * TM, TM), TM)

            for i in range(dh // TN):
                cs = slice(i * TN, (i + 1) * TN)
                ws = slice(base + i * 2 * size, base + (i + 1) * 2 * size)
                acc[rs, cs] += jnp.dot(z[rs, g * 2 * TN:g * 2 * TN + 2 * size], wt[ws, :], preferred_element_type=jnp.float32)
            if drain:
                drain(t, rs)
            return carry

        lax.fori_loop(0, n_mb * tok // TM, tile, 0)

    def out_copy(t, buf, sem):
        m, q = t // (tok // TM), lax.rem(t, tok // TM)
        return pltpu.make_async_copy(buf, y_out.at[m, pl.ds(pl.multiple_of(q * TM, TM), TM)], sem)

    def drain_tile(t, rs):
        for p, buf in enumerate((ln_a, ln_b)):
            @pl.when(lax.rem(t, 2) == p)
            def _():
                @pl.when(t >= 2)
                def _():
                    out_copy(t - 2, buf, osem.at[p]).wait()
                buf[...] = acc[rs, :].astype(jnp.bfloat16)
                out_copy(t, buf, osem.at[p]).start()

    def start(copies):
        for cp in copies:
            cp.start()

    def finish(copies):
        for cp in copies:
            cp.wait()

    def chunk(p, c, piece, drain=None):
        size = piece[1]
        own = w2_copies(p, size, 0, True, row, 0)
        start(own)

        def wait_h():
            if not isinstance(c, int):
                @pl.when(c < EARLY // 2)
                def _():
                    for m in range(n_mb):
                        for k in range(2):
                            h_early(m, 2 * c + k).wait_recv()

                @pl.when(c >= EARLY // 2)
                def _():
                    for k in range(2):
                        h_pair(2 * c + k).wait_recv()
            elif c == n2 - 1:
                for k in range(2):
                    h_last(k, last_at.index(piece[0])).wait_recv()
            elif piece[0] == 0:
                for k in range(2):
                    h_pair(2 * c + k).wait_recv()

        w2_sib(p).wait_recv()
        sib_w = w2_copies(p, size, 0, False, sib, 1)
        start(sib_w)
        h0 = h_copies(c, piece, 0)
        h1 = h_copies(c, piece, 1)
        x_w = w2_copies(p, size, 1, False, xn, 2)
        f_w = w2_copies(p, size, 1, False, xs_row, 3)

        def near_half():
            finish(own)
            finish(sib_w)
            finish(h0)
            product(size, 0)

        @pl.when(diagonal)
        def _():
            start(h0)
            near_half()

        @pl.when(jnp.logical_not(diagonal))
        def _():
            start(h1)

        w2_x(p).wait_recv()
        w2_fwd(p).start()
        start(x_w)
        wait_h()

        @pl.when(diagonal)
        def _():
            start(h1)

        @pl.when(jnp.logical_not(diagonal))
        def _():
            start(h0)
            near_half()

        w2_fwd(p).wait_recv()
        start(f_w)
        finish(h1)
        finish(x_w)
        finish(f_w)
        product(size, 1, drain)

    def middle(c, carry):
        chunk(c, c, (0, TN))

        @pl.when(c == 0)
        def _():
            for p in range(full, full + len(TAIL)):
                w2_x(p).start()
                w2_sib(p).start()

        return carry

    lax.fori_loop(0, full, middle, 0)
    for i, (back, at, size) in enumerate(TAIL):
        chunk(full + i, n2 - back, (at, size), drain_tile if i == len(TAIL) - 1 else None)
    steps = n_mb * tok // TM
    for p, buf in enumerate((ln_a, ln_b)):
        out_copy(steps - 2 + p, buf, osem.at[p]).wait()

    g_move().wait_send()
    for m in range(n_mb):
        x_move(m).wait_send()

    def sent1(s, carry):
        w1_x(s).wait_send()
        w1_sib(s).wait_send()
        w1_fwd(s).wait_send()
        return carry

    def sent2(c, carry):
        w2_x(c).wait_send()
        w2_sib(c).wait_send()
        w2_fwd(c).wait_send()
        return carry

    def sent_early(s, carry):
        for m in range(n_mb):
            h_early(m, s).wait_send()
        return carry

    def sent_pair(s, carry):
        h_pair(s).wait_send()
        return carry

    lax.fori_loop(0, nq, sent1, 0)
    lax.fori_loop(0, full, sent2, 0)
    for p in range(full, full + len(TAIL)):
        sent2(p, 0)
    lax.fori_loop(0, EARLY, sent_early, 0)
    lax.fori_loop(EARLY, n1 - 2, sent_pair, 0)
    for u in range(len(LAST)):
        for k in range(2):
            h_last(k, u).wait_send()


def solution(mesh):
    act_spec = P(None, ("dp", "row"), "col")

    def per_device(x, gamma, w1, w2):
        n_mb, tok, dh = x.shape
        d4, hid = w1.shape
        r4 = w2.shape[0]
        n1, n2 = hid // TN, r4 // TN
        n2p = n2 - TAIL[0][0] + len(TAIL)
        nh = (n_mb - 1) * EARLY + n1 - 2 + 2 * len(LAST)
        bf16, f32 = jnp.bfloat16, jnp.float32
        dma = pltpu.SemaphoreType.DMA
        any_spec = pl.BlockSpec(memory_space=pl.ANY)
        shapes = (
            jax.ShapeDtypeStruct((n_mb, tok, dh), bf16),
            jax.ShapeDtypeStruct((n_mb, tok, dh), bf16),
            jax.ShapeDtypeStruct((dh // 128, 128), f32),
            jax.ShapeDtypeStruct((4, hid // TW, d4, TW), bf16),
            jax.ShapeDtypeStruct((4, r4, dh), bf16),
            jax.ShapeDtypeStruct((2, n1, n_mb, TN // SUB, tok, SUB), bf16),
        )
        outs = pl.pallas_call(
            functools.partial(kernel, (n_mb, tok, dh, d4, hid, r4)),
            out_shape=shapes,
            in_specs=[any_spec] * 4,
            out_specs=[any_spec] * len(shapes),
            scratch_shapes=[
                pltpu.VMEM((n_mb * tok, 2 * dh), bf16),
                pltpu.VMEM((8 * d4, TN), bf16),
                pltpu.VMEM((tok, TN), bf16),
                pltpu.VMEM((TM, dh), bf16),
                pltpu.VMEM((TM, dh), bf16),
                pltpu.VMEM((2, dh // 128, 128), f32),
                pltpu.VMEM((2, dh), f32),
                pltpu.VMEM((n_mb * tok, dh), f32),
                dma((n_mb,)), dma((n_mb,)), dma((2,)),
                *[dma((hid // TW,))] * 6,
                dma((n2p,)), dma((n2p,)), dma((n2p,)), dma((n2p,)), dma((n2p,)), dma((n2p,)),
                dma((nh,)), dma((nh,)),
                dma((8,)), dma((8 * (TN // SUB),)), dma((2,)), dma((4 * (dh // TN),)),
            ],
            compiler_params=pltpu.CompilerParams(collective_id=0, has_side_effects=True, vmem_limit_bytes=67043328),
        )(x, gamma.reshape(dh // 128, 128), w1, w2)
        return outs[0]

    return jax.shard_map(per_device, mesh=mesh, in_specs=(act_spec, P("col"), P("row", "col"), P("row", "col")), out_specs=act_spec, check_vma=False)
```
